32 devices in a mesh: lat: 4 (over z), lon: 8 (over y, x, core).
Axes of the slice: x: 2, y: 2, z: 4, core: 2. Of those that a mesh axis runs over, the one named last changes fastest.
Arguments:
- observations: bfloat16 [49152, 128], P(('lat', 'lon')), may hold values from -6 to 6
- owner_device: int32 [49152, 1], P(('lat', 'lon')), may hold values from 0 to 31; in each aligned block of 1536 rows (0 to 1535, 1536 to 3071, ...) at most 96 rows name the same one
- local_cell: int32 [49152], P(('lat', 'lon')), may hold values from 0 to 383
- valid_counts: int32 [32], P(('lat', 'lon')), may hold values from 768 to 1536
- weight_in: bfloat16 [128, 256], replicated, may hold values from -0.5 to 0.5
- bias_in: float32 [256], replicated, may hold values from -3 to 3
- weight_out: bfloat16 [256, 256], replicated, may hold values from -0.375 to 0.375
- kernel_taps: float32 [9, 256], replicated, may hold values from -2 to 2
- cotangent: bfloat16 [64, 192, 256], P(('lat', 'lon')), may hold values from -6 to 6
Outputs:
- grid_out: bfloat16 [64, 192, 256], P(('lat', 'lon'))
- grad_weight_in: float32 [128, 256], replicated
- grad_bias_in: float32 [256], replicated
- grad_weight_out: float32 [256, 256], replicated
- grad_kernel: float32 [9, 256], replicated
The draws below stay inside these ranges and needn't reach their ends.
Inputs may be any that keep to these rules, and one draw needn't show every extreme that they name: `owner_device`: within the rows of one block, at most 96 rows name one owner, and in every draw some block names some owner exactly 96 times.
All inputs are finite; a program needn't handle non-finite values.
Results may differ from the reference program's by a relative error of at most 0.0065.
Values may be sent and summed in bfloat16 or wider, within the bound.
A program may use at most 64 MiB of HBM per device.

```python
import math
import jax
import jax.numpy as jnp
import numpy as np
from jax import lax

FEAT = 128
HIDDEN_SIZE = 256
CHANNELS = 256
TAPS = 9
TLAT = 16
TLON = 24
OBS_DEV = 1536
GLAT = 64
GLON = 192
OBS_ALL = 49152
CAP = 96
N_LAT = 4
N_LON = 8


def with_ends(result, rng, low, high):
    extent = result.shape
    spot = [jax.random.randint(jax.random.fold_in(rng, axis), (), 0, extent[axis]) for axis in range(len(extent))]
    result = result.at[tuple(spot)].set(low)
    longest = extent.index(max(extent))
    spot[longest] = (spot[longest] + 1) % extent[longest]
    return result.at[tuple(spot)].set(high)


def levels(rng, shape, shards, least, top_value):
    factor_of, own = 1.0, jax.random.fold_in(rng, 6)
    for axis_at, parts in shards:
        heights = jnp.exp(jax.random.uniform(jax.random.fold_in(own, axis_at), (parts,), jnp.float32, least / len(shards), top_value / len(shards)))
        factor_of = factor_of * jnp.repeat(heights, shape[axis_at] // parts).reshape([-1 if axis == axis_at else 1 for axis in range(len(shape))])
    return factor_of


def deal_out(stream_key, own, number, rows, count, top, reach, slope):
    sequence = jax.random.permutation(stream_key, count)
    packed, ordinary = portions_of(count, rows * top, reach, slope, True), portions_of(count, rows * top, reach, slope, False)
    places = jnp.arange(count)

    def named(sizes, turn):
        used = int((sizes > 0).sum())
        fixed = max(1, used // 4)
        shifted = fixed + (places - fixed + turn * (used - fixed)) % max(1, count - fixed)
        return jnp.zeros((count,), jnp.int32).at[sequence[jnp.where(places < fixed, places, shifted)]].set(jnp.asarray(sizes, jnp.int32))

    sizes = jnp.where(number % 4 == 0, named(packed, number // 4), named(ordinary, number - number // 4 - 1))
    mixed = jax.random.permutation(jax.random.fold_in(own, 3), count)
    source_of, taker = mixed[0:count // 2 * 2:2], mixed[1:count // 2 * 2:2]
    room = jnp.minimum(sizes[source_of] - 1, reach - sizes[taker]) // 2
    room = jnp.where((source_of == sequence[0]) | (taker == sequence[0]) | (sizes[taker] == 0), 0, jnp.maximum(room, 0))
    shifted = jax.random.randint(jax.random.fold_in(own, 4), (count // 2,), 0, 1 << 20) % (room + 1)
    sizes = sizes.at[source_of].add(-shifted).at[taker].add(shifted)
    items = jnp.searchsorted(jnp.cumsum(sizes), jnp.arange(rows * top), side="right").astype(jnp.int32)
    grid = items.reshape(top, rows).T
    grid = grid[jax.random.permutation(jax.random.fold_in(own, 1), rows)]
    turn = jax.random.randint(jax.random.fold_in(own, 2), (rows, 1), 0, top)
    return jnp.take_along_axis(grid, (jnp.arange(top)[None, :] + turn) % top, axis=1)


def portions_of(amount, total, limit, lean, full):
    weights = [(1 << 20) // math.isqrt(standing ** lean) + 1 for standing in range(1, amount + 1)]
    largest = limit if full else min(limit, max(-(-total // amount), total * weights[0] // sum(weights)))
    least = 1 if total - largest >= amount - 1 else 0
    counts, surplus = [largest] + [least] * (amount - 1), total - largest - least * (amount - 1)
    while surplus > 0:
        movable = [i for i in range(1, amount) if counts[i] < largest] or [i for i in range(1, amount) if counts[i] < limit]
        whole, left = sum([weights[i] for i in movable]), surplus
        for i in movable:
            extra = min(limit - counts[i], max(1, left * weights[i] // whole), surplus)
            counts[i] = counts[i] + extra
            surplus = surplus - extra
    return np.array(counts)


def bell_draw(own_key, shape, width, bound, split=(), kind=jnp.bfloat16):
    array = width * jax.random.normal(own_key, shape, jnp.float32)
    if split:
        array = array * levels(own_key, shape, split, -0.22, 0.18)
    return jnp.clip(array, -bound, bound).astype(kind)


def setup_inputs(seed: int = 0) -> dict:
    splits = jax.random.split(jax.random.key(seed), 10)
    observations = bell_draw(splits[0], (OBS_ALL, FEAT), 1.0, 6.0, ((0, 32),))
    owner_device_keys = jax.random.split(jax.random.fold_in(splits[1], 1), OBS_ALL // OBS_DEV)
    owner_device_turns = jax.random.permutation(jax.random.fold_in(splits[1], 3), OBS_ALL // OBS_DEV)
    owner_device = jax.vmap(lambda own, number: deal_out(jax.random.fold_in(splits[1], 2), own, number, OBS_DEV, N_LAT * N_LON, 1, CAP, 2))(owner_device_keys, owner_device_turns).reshape((OBS_ALL, 1))
    local_cell = with_ends(jax.random.randint(splits[2], (OBS_ALL,), 0, TLAT * TLON), jax.random.fold_in(splits[2], 1), 0, (TLAT * TLON) - 1).astype(jnp.int32)
    valid_counts = with_ends(jax.random.randint(splits[3], (N_LAT * N_LON,), OBS_DEV // 2, OBS_DEV + 1), jax.random.fold_in(splits[3], 1), OBS_DEV // 2, OBS_DEV).astype(jnp.int32)
    weight_in = bell_draw(splits[4], (FEAT, HIDDEN_SIZE), FEAT ** -0.5, 0.5)
    bias_in = bell_draw(splits[5], (HIDDEN_SIZE,), 0.5, 3.0, (), jnp.float32)
    weight_out = bell_draw(splits[6], (HIDDEN_SIZE, CHANNELS), HIDDEN_SIZE ** -0.5, 0.375)
    kernel_taps = bell_draw(splits[7], (TAPS, CHANNELS), 0.33, 2.0, (), jnp.float32)
    cotangent = bell_draw(splits[8], (GLAT, GLON, CHANNELS), 1.0, 6.0, ((0, 32),))
    return {"observations": observations, "owner_device": owner_device, "local_cell": local_cell, "valid_counts": valid_counts, "weight_in": weight_in, "bias_in": bias_in, "weight_out": weight_out, "kernel_taps": kernel_taps, "cotangent": cotangent}


OFFSETS = [(shift_lat, shift_lon) for shift_lat in (-1, 0, 1) for shift_lon in (-1, 0, 1)]

def pad_grid(values):
    wrapped = jnp.concatenate([values[:, -1:], values, values[:, :1]], axis=1)
    return jnp.pad(wrapped, ((1, 1), (0, 0), (0, 0)))

def encoder(rows, weight_in, bias_in, weight_out):
    before = jnp.dot(rows, weight_in, preferred_element_type=jnp.float32) + bias_in
    hidden = jax.nn.gelu(before).astype(jnp.bfloat16)
    encoded = jnp.dot(hidden, weight_out, preferred_element_type=jnp.float32).astype(jnp.bfloat16)
    return (before, hidden, encoded)

def local_grads(rows, before, hidden, upstream, weight_out):
    contract = (((0,), (0,)), ((), ()))
    grad_out = lax.dot_general(hidden, upstream, contract, preferred_element_type=jnp.float32)
    back = lax.dot_general(upstream, weight_out, (((1,), (1,)), ((), ())), preferred_element_type=jnp.float32)
    _, pullback = jax.vjp(jax.nn.gelu, before)
    pre_grad = pullback(back)[0].astype(jnp.bfloat16)
    grad_in = lax.dot_general(rows, pre_grad, contract, preferred_element_type=jnp.float32)
    grad_bias = lax.optimization_barrier(jnp.sum(pre_grad.astype(jnp.float32), axis=0))
    return (grad_in, grad_bias, grad_out)

def reference(observations, owner_device, local_cell, valid_counts, weight_in, bias_in, weight_out, kernel_taps, cotangent):
    devices_all = N_LAT * N_LON
    cells_total = GLAT * GLON
    row_blocks = observations.reshape(devices_all, OBS_DEV, FEAT)
    owner_blocks = owner_device.reshape(devices_all, OBS_DEV)
    local_blocks = local_cell.reshape(devices_all, OBS_DEV)

    def destination(owner_row, local_row, count):
        valid_rows = jnp.arange(OBS_DEV, dtype=jnp.int32) < count
        lat_cell = owner_row // N_LON * TLAT + local_row // TLON
        lon_cell = owner_row % N_LON * TLON + local_row % TLON
        return jnp.where(valid_rows, lat_cell * GLON + lon_cell, cells_total).astype(jnp.int32)

    def forward_step(deposit, item):
        rows, owner_row, local_row, count = item
        target = destination(owner_row, local_row, count)
        _, _, encoded = encoder(rows, weight_in, bias_in, weight_out)
        deposit = deposit + jax.ops.segment_sum(encoded.astype(jnp.float32), target, num_segments=cells_total + 1)
        return (deposit, None)
    deposit, _ = lax.scan(forward_step, jnp.zeros((cells_total + 1, CHANNELS), jnp.float32), (row_blocks, owner_blocks, local_blocks, valid_counts))
    point = deposit[:cells_total].reshape(GLAT, GLON, CHANNELS)
    padded = pad_grid(point)
    grid_field = jnp.zeros((GLAT, GLON, CHANNELS), jnp.float32)
    for tap_index, (shift_lat, shift_lon) in enumerate(OFFSETS):
        window = padded[1 + shift_lat:1 + shift_lat + GLAT, 1 + shift_lon:1 + shift_lon + GLON]
        grid_field = grid_field + kernel_taps[tap_index] * window
    grid_out = grid_field.astype(jnp.bfloat16)
    loss_scale = 1.0 / math.sqrt(OBS_DEV * devices_all)
    cot_float = cotangent.astype(jnp.float32)
    cot_padded = pad_grid(cot_float)
    kernel_rows = []
    adjoint = jnp.zeros((GLAT, GLON, CHANNELS), jnp.float32)
    for tap_index, (shift_lat, shift_lon) in enumerate(OFFSETS):
        window = padded[1 + shift_lat:1 + shift_lat + GLAT, 1 + shift_lon:1 + shift_lon + GLON]
        kernel_rows.append(loss_scale * lax.optimization_barrier(jnp.sum(cot_float * window, axis=(0, 1))))
        back_window = cot_padded[1 - shift_lat:1 - shift_lat + GLAT, 1 - shift_lon:1 - shift_lon + GLON]
        adjoint = adjoint + kernel_taps[tap_index] * back_window
    grad_kernel = jnp.stack(kernel_rows)
    adjoint = (loss_scale * adjoint).astype(jnp.bfloat16)
    adjoint_rows = jnp.concatenate([adjoint.reshape(cells_total, CHANNELS), jnp.zeros((1, CHANNELS), jnp.bfloat16)], axis=0)

    def backward_step(totals, item):
        rows, owner_row, local_row, count = item
        target = destination(owner_row, local_row, count)
        before, hidden, _ = encoder(rows, weight_in, bias_in, weight_out)
        upstream = adjoint_rows[target]
        grads = local_grads(rows, before, hidden, upstream, weight_out)
        return (tuple((total + grad for total, grad in zip(totals, grads))), None)
    zeros_start = (jnp.zeros((FEAT, HIDDEN_SIZE), jnp.float32), jnp.zeros((HIDDEN_SIZE,), jnp.float32), jnp.zeros((HIDDEN_SIZE, CHANNELS), jnp.float32))
    totals, _ = lax.scan(backward_step, zeros_start, (row_blocks, owner_blocks, local_blocks, valid_counts))
    return (grid_out, totals[0], totals[1], totals[2], grad_kernel)
```

```python
import functools
import math

import jax
import jax.numpy as jnp
from jax import lax
from jax.experimental import pallas as pl
from jax.experimental.pallas import tpu as pltpu
from jax.sharding import PartitionSpec as P

MESH = pl.DeviceIdType.MESH
F32 = jnp.float32
BF16 = jnp.bfloat16
OFFSETS = [(a, b) for a in (-1, 0, 1) for b in (-1, 0, 1)]
CURVE = math.sqrt(2.0 / math.pi)
BEND = 0.044715
META = 8
EDGE = 8
STEP_ROWS = 384
EARLY = 4


def round_up(value, step):
    return -(-value // step) * step


def iota(shape, dim):
    return lax.broadcasted_iota(jnp.int32, shape, dim)


def dot(left, right, contract=((1,), (0,))):
    return lax.dot_general(left, right, (contract, ((), ())), preferred_element_type=F32)


def split_of(n_lat):
    return 2 if n_lat % 2 == 0 and n_lat >= 4 else 1


def kernel(
    n_lat, n_lon, split, slots, batch, scale,
    obs_h, owner_h, cell_h, count, w_in_h, b_in_h, w_out_h, taps_h, cot_h,
    main_o, top_o, bot_o, sums_o, misc_o,
    obs, owner, cell, w_in, b_in, w_out, taps, cot,
    meta, slot_row, sbuf, rbuf, cot_s, cot_e, cot_r, cot_top, cot_bot, c32, adj_f, adj_b,
    dep, moved, con_s, con_e, gka, total, bias, tot_b, rs_r, z_s, z_r, fin_s, misc_s, misc_r, misc_z,
    in_sem, row_send, row_recv, cot_send, cot_recv, edge_send, top_recv, bot_recv,
    con_send, con_recv, rim_send, rim_recv, rs_send, rs_recv, z_send, z_recv, ag_send, ag_recv,
    mp_send, mp_recv, mz_send, mz_recv,
):
    n = n_lat * n_lon
    lat, lon = lax.axis_index("lat"), lax.axis_index("lon")
    me = lat * n_lon + lon
    deep = n_lat // split
    group, level = lat // deep, lax.rem(lat, deep)
    peers = n // split
    obs_rows, feat = obs.shape
    own_rows, cols, channels = cot.shape
    tile_rows, tile_cols = own_rows * n_lon, cols // n_lon
    cells = tile_rows * tile_cols
    wide = tile_cols + EDGE
    hidden_size = w_in.shape[1]
    piece = tot_b.shape[1]
    holders = split * n_lon
    scope = jax.named_scope

    def place(target):
        return (target // n_lon, lax.rem(target, n_lon))

    def partner(off):
        return (group * deep + lax.rem(level + lax.rem(off, deep), deep), lax.rem(lon + off // deep, n_lon))

    def tile_lat(h):
        return h * deep + level

    def remote(src, dst, send, recv, device):
        return pltpu.make_async_remote_copy(
            src_ref=src, dst_ref=dst, send_sem=send, recv_sem=recv,
            device_id=device, device_id_type=MESH,
        )

    def drain(ref, sem):
        pltpu.make_async_copy(ref, ref, sem).wait()

    pairs = [
        (owner_h, owner), (cell_h, cell), (obs_h, obs), (cot_h, cot),
        (w_in_h, w_in), (b_in_h, b_in), (w_out_h, w_out), (taps_h, taps),
    ]
    fetches = [pltpu.make_async_copy(src, dst, in_sem.at[i]) for i, (src, dst) in enumerate(pairs)]
    for fetch in fetches:
        fetch.start()

    barrier = pltpu.get_barrier_semaphore()

    def greet(off, carry):
        pl.semaphore_signal(
            barrier, inc=1, device_id=place(lax.rem(me + off, n)), device_id_type=MESH
        )
        return carry

    with scope("greet"):
        lax.fori_loop(1, n, greet, 0)

    with scope("zero"):
        for h in range(split):
            @pl.when(tile_lat(h) == 0)
            def _(h=h):
                cot_top[h] = jnp.zeros((wide, channels), BF16)

            @pl.when(tile_lat(h) == n_lat - 1)
            def _(h=h):
                cot_bot[h] = jnp.zeros((wide, channels), BF16)

            for b in range(3):
                for i in (0, 1, tile_rows + 2, tile_rows + 3):
                    moved[h, b, i] = jnp.zeros((wide, channels), F32)

        has_top = jnp.logical_and(lon == 0, lat > 0)
        has_bot = jnp.logical_and(lon == n_lon - 1, lat < n_lat - 1)

        @pl.when(jnp.logical_not(has_top))
        def _():
            top_o[...] = jnp.zeros_like(top_o)

        @pl.when(jnp.logical_not(has_bot))
        def _():
            bot_o[...] = jnp.zeros_like(bot_o)

        dep[...] = jnp.zeros_like(dep)
        total[...] = jnp.zeros_like(total)
        bias[...] = jnp.zeros_like(bias)
        gka[...] = jnp.zeros_like(gka)

    with scope("meta"):
        fetches[0].wait()
        own_row = owner[...]
        match = (own_row == iota((n, obs_rows), 0)).astype(F32)
        block = 256 if obs_rows % 256 == 0 else 128
        upper = (iota((block, block), 0) < iota((block, block), 1)).astype(F32).astype(BF16)
        carry = jnp.zeros((n, 1), F32)
        ranks = []
        for start in range(0, obs_rows, block):
            part = match[:, start:start + block]
            before = dot(part.astype(BF16), upper) + carry
            ranks.append(jnp.sum(before * part, axis=0, keepdims=True))
            carry = carry + jnp.sum(part, axis=1, keepdims=True)
        rank = jnp.concatenate(ranks, axis=1).astype(jnp.int32)
        slot_row[...] = own_row * slots + rank
        fetches[1].wait()
        lane = iota((1, obs_rows), 1)
        cells_row = jnp.concatenate([cell[i:i + 1, :] for i in range(obs_rows // 128)], axis=1)
        code = jnp.where(lane < count[0], cells_row + 1, 0)
        high = (code // 128).astype(F32)
        low = lax.rem(code, 128).astype(F32)
        coded = jnp.concatenate([match * high, match * low], axis=0).astype(BF16)
        by_rank = (rank == iota((128, obs_rows), 0)).astype(F32).astype(BF16)
        meta[...] = dot(coded, by_rank, ((1,), (1,)))
        fetches[2].wait()

    per_step = batch // split
    steps = peers // per_step

    def prepare(s, carry):
        ids = slot_row[...]
        picks = []
        for u in range(batch):
            to_lat, to_lon = partner(s * per_step + u // split)
            target = ((u % split) * deep + lax.rem(to_lat, deep)) * n_lon + to_lon
            rel = jnp.clip(ids - target * slots, -1, slots).astype(F32)
            rel = jnp.broadcast_to(rel, (16, obs_rows)).astype(BF16)
            for at in range(0, slots, 16):
                line = (iota((16, obs_rows), 0) + at).astype(F32).astype(BF16)
                picks.append(jnp.where(rel == line, jnp.ones_like(line), jnp.zeros_like(line)))
        rows = dot(jnp.concatenate(picks, axis=0), obs[...]).astype(BF16)
        line = iota((META, 128), 0)
        for q in range(per_step):
            off = s * per_step + q
            to_lat, to_lon = partner(off)
            tail = jnp.zeros((META, 128), F32)
            for h in range(split):
                target = (h * deep + lax.rem(to_lat, deep)) * n_lon + to_lon
                u = q * split + h
                sbuf[off, h * slots:(h + 1) * slots, :] = rows[u * slots:(u + 1) * slots]
                tail = jnp.where(line == 2 * h, meta[pl.ds(target, 1), :], tail)
                tail = jnp.where(line == 2 * h + 1, meta[pl.ds(n + target, 1), :], tail)
            sbuf[off, split * slots:split * slots + META, :] = tail.astype(BF16)
        return carry

    takers = batch

    def ship_one(off):
        remote(sbuf.at[off], rbuf.at[off], row_send, row_recv.at[off // takers], partner(off)).start()

    def ship(s, carry):
        for q in range(per_step):
            ship_one(s * per_step + q)
        return carry

    early = min(EARLY, steps)
    with scope("prep0"):
        lax.fori_loop(0, early, prepare, 0)

    with scope("cotprep"):
        fetches[3].wait()
        rim = iota((EDGE, channels), 0)
        rows_f = [cot[y].astype(F32) for y in range(own_rows)]
        for j in range(n_lon):
            start, stop = j * tile_cols, (j + 1) * tile_cols
            after, ahead = stop % cols, (start - EDGE) % cols
            mixed = jnp.zeros((EDGE, channels), F32)
            for y in range(own_rows):
                row = rows_f[y]
                ends = jnp.where(
                    rim == 0, row[after:after + EDGE],
                    jnp.where(rim == EDGE - 1, row[ahead:ahead + EDGE], 0.0),
                )
                cot_s[j, y * tile_cols:(y + 1) * tile_cols, :] = cot[y, start:stop, :]
                mixed = mixed + (pltpu.roll(ends, EDGE - 2 * y, 0) if y else ends)
                if y == 0:
                    cot_e[0, j, 0:tile_cols, :] = cot[y, start:stop, :]
                    cot_e[0, j, tile_cols:wide, :] = ends.astype(BF16)
                if y == own_rows - 1:
                    cot_e[1, j, 0:tile_cols, :] = cot[y, start:stop, :]
                    cot_e[1, j, tile_cols:wide, :] = ends.astype(BF16)
            cot_s[j, own_rows * tile_cols:own_rows * tile_cols + EDGE, :] = mixed.astype(BF16)

    with scope("barw"):
        pl.semaphore_wait(barrier, n - 1)

    def hop(step):
        return lax.rem(lon + step, n_lon)

    def side(turn):
        return lax.rem(group + turn, split)

    with scope("ship"):
        for turn in range(split - 1, -1, -1):
            to_lat = side(turn) * deep + level
            for step in range(n_lon):
                if turn or step:
                    other = hop(step)
                    remote(
                        cot_s.at[other], cot_r.at[group * n_lon + lon], cot_send, cot_recv, (to_lat, other)
                    ).start()
        cot_r[group * n_lon + lon] = cot_s[lon]

        @pl.when(jnp.logical_and(lon == n_lon - 1, lat < n_lat - 1))
        def _():
            to_tile = lat + 1
            for turn in range(split):
                for j in range(n_lon):
                    remote(
                        cot_e.at[1, j], cot_top.at[to_tile // deep], edge_send, top_recv.at[to_tile // deep],
                        (turn * deep + lax.rem(to_tile, deep), j),
                    ).start()

        @pl.when(jnp.logical_and(lon == 0, lat > 0))
        def _():
            to_tile = lat - 1
            for turn in range(split):
                for j in range(n_lon):
                    remote(
                        cot_e.at[0, j], cot_bot.at[to_tile // deep], edge_send, bot_recv.at[to_tile // deep],
                        (turn * deep + lax.rem(to_tile, deep), j),
                    ).start()

        pltpu.make_async_copy(sbuf.at[0], rbuf.at[0], row_recv.at[0]).start()
        for q in range(1, per_step):
            ship_one(q)
        lax.fori_loop(1, early, ship, 0)

    with scope("prep1"):
        if early < steps:
            lax.fori_loop(early, steps, lambda s, c: ship(s, prepare(s, c)), 0)

    with scope("cotwait"):
        for fetch in fetches[4:]:
            fetch.wait()
        drain(cot_r.at[pl.ds(0, holders - 1)], cot_recv)
        for h in range(split):
            @pl.when(tile_lat(h) > 0)
            def _(h=h):
                drain(cot_top.at[h], top_recv.at[h])

            @pl.when(tile_lat(h) < n_lat - 1)
            def _(h=h):
                drain(cot_bot.at[h], bot_recv.at[h])

    with scope("adjoint"):
        tap = taps[...]
        half = channels // 2
        for h in range(split):
            c32[h, 0] = cot_top[h].astype(F32)
            c32[h, tile_rows + 1] = cot_bot[h].astype(F32)

            def widen(j, carry, h=h):
                at = h * n_lon + j
                ends = cot_r[at, own_rows * tile_cols:own_rows * tile_cols + EDGE, :].astype(F32)
                for r in range(own_rows):
                    m = j * own_rows + r + 1
                    c32[h, m, 0:tile_cols, :] = cot_r[at, r * tile_cols:(r + 1) * tile_cols, :].astype(F32)
                    c32[h, m, tile_cols:wide, :] = pltpu.roll(ends, 2 * r, 0) if r else ends
                return carry

            lax.fori_loop(0, n_lon, widen, 0)

            def adjoin(m, carry, h=h):
                for c in range(0, channels, half):
                    acc = jnp.zeros((tile_cols, half), F32)
                    for a in (-1, 0, 1):
                        row = c32[h, m + 1 - a, :, c:c + half]
                        for b in (-1, 0, 1):
                            k = 3 * (a + 1) + b + 1
                            turned = pltpu.roll(row, b % wide, 0) if b else row
                            acc = acc + tap[k:k + 1, c:c + half] * turned[0:tile_cols]
                    adj_f[pl.ds(pl.multiple_of(m * tile_cols, 8), tile_cols), c:c + half] = scale * acc
                return carry

            lax.fori_loop(0, tile_rows, adjoin, 0)
            adj_b[h] = adj_f[...].astype(BF16)

    def take(t, carry):
        first = t * takers
        with scope("rowwait"):
            drain(rbuf.at[pl.ds(first, takers)], row_recv.at[t])
        rows = jnp.concatenate(
            [rbuf[first + q, h * slots:(h + 1) * slots, :] for h in range(split) for q in range(takers)], axis=0
        )
        x = dot(rows, w_in[...]) + b_in[...]
        square = x * x
        t_val = jnp.tanh(x * (CURVE + (CURVE * BEND) * square))
        upper_half = 0.5 + 0.5 * t_val
        lower_half = 0.5 - 0.5 * t_val
        active = x * upper_half
        hidden = active.astype(BF16)
        slope = upper_half + (active * lower_half) * (2.0 * CURVE + (6.0 * CURVE * BEND) * square)
        encoded = dot(hidden, w_out[...]).astype(BF16)
        share = takers * slots
        ups = []
        for h in range(split):
            codes = []
            for q in range(takers):
                tail = rbuf[first + q, split * slots:split * slots + META, :].astype(F32)
                codes.append((128.0 * tail[2 * h:2 * h + 1] + tail[2 * h + 1:2 * h + 2])[:, 0:slots])
            codes = jnp.concatenate(codes, axis=1).astype(jnp.int32)
            pick = (codes == iota((cells, share), 0) + 1).astype(F32).astype(BF16)
            dep[h] += dot(pick, encoded[h * share:(h + 1) * share])
            ups.append(dot(pick, adj_b[h], ((0,), (0,))).astype(BF16))
        upstream = jnp.concatenate(ups, axis=0)
        back = dot(upstream, w_out[...], ((1,), (1,)))
        pre = (back * slope).astype(BF16)
        total[0:hidden_size, :] += dot(hidden, upstream, ((0,), (0,)))
        total[hidden_size:hidden_size + feat, :] += dot(rows, pre, ((0,), (0,)))
        bias[...] += jnp.sum(pre.astype(F32), axis=0, keepdims=True)
        return carry

    with scope("take"):
        lax.fori_loop(0, peers // takers, take, 0)

    with scope("rssend"):
        for p in range(n_lon):
            tot_b[p] = total[p * piece:(p + 1) * piece, :].astype(BF16)
        for step in range(1, n_lon):
            remote(tot_b.at[hop(step)], rs_r.at[lon], rs_send, rs_recv, (lat, hop(step))).start()

    def spread(h):
        def turn_row(m, carry):
            row = dep[h, pl.ds(pl.multiple_of(m * tile_cols, 8), tile_cols), :]
            row = jnp.concatenate([row, jnp.zeros((EDGE, channels), F32)], axis=0)
            moved[h, 0, m + 2] = pltpu.roll(row, 1, 0)
            moved[h, 1, m + 2] = row
            moved[h, 2, m + 2] = pltpu.roll(row, wide - 1, 0)
            return carry

        lax.fori_loop(0, tile_rows, turn_row, 0)

        def out_row(i, c):
            acc = jnp.zeros((wide, half), F32)
            seen = c32[h, i, :, c:c + half]
            for a in (-1, 0, 1):
                for b in (-1, 0, 1):
                    k = 3 * (a + 1) + b + 1
                    value = moved[h, b + 1, i + 1 + a, :, c:c + half]
                    acc = acc + tap[k:k + 1, c:c + half] * value
                    prod = seen * value
                    folded = prod[0:8]
                    for at in range(8, wide, 8):
                        folded = folded + prod[at:at + 8]
                    gka[k, :, c:c + half] += folded
            return acc

        def strip(j, carry):
            for c in range(0, channels, half):
                mixed = jnp.zeros((EDGE, half), F32)
                for r in range(own_rows):
                    acc = out_row(j * own_rows + r + 1, c)
                    con_s[h, j, r * tile_cols:(r + 1) * tile_cols, c:c + half] = acc[0:tile_cols].astype(BF16)
                    ends = acc[tile_cols:wide]
                    mixed = mixed + (pltpu.roll(ends, EDGE - 2 * r, 0) if r else ends)
                con_s[h, j, own_rows * tile_cols:own_rows * tile_cols + EDGE, c:c + half] = mixed.astype(BF16)
            return carry

        for e, i in ((0, 0), (1, tile_rows + 1)):
            for c in range(0, channels, half):
                con_e[h, e, :, c:c + half] = out_row(i, c).astype(BF16)
        lax.fori_loop(0, n_lon, strip, 0)

    def send_strip(h, step):
        other = hop(step)
        remote(
            con_s.at[h, other], main_o.at[group * n_lon + lon], con_send, con_recv, (tile_lat(h), other)
        ).start()

    def rim_copy(h, e):
        where = group * n_lon + lon
        if e == 0:
            return remote(con_e.at[h, 0], bot_o.at[where], rim_send, rim_recv.at[0], (tile_lat(h) - 1, n_lon - 1))
        return remote(con_e.at[h, 1], top_o.at[where], rim_send, rim_recv.at[1], (tile_lat(h) + 1, 0))

    def send_rims(h):
        @pl.when(tile_lat(h) > 0)
        def _():
            rim_copy(h, 0).start()

        @pl.when(tile_lat(h) < n_lat - 1)
        def _():
            rim_copy(h, 1).start()

    first_part = n_lon // 2
    with scope("spread"):
        for turn in range(1, split):
            h = side(turn)
            spread(h)
            send_rims(h)
            for step in range(first_part):
                send_strip(h, step)
        spread(group)
        send_rims(group)

    with scope("misc"):
        grads = [jnp.sum(gka[k], axis=0, keepdims=True) * scale for k in range(len(OFFSETS))]
        spare = misc_s.shape[0] - len(OFFSETS) - 1
        misc_s[...] = jnp.concatenate(
            [bias[...]] + grads + [jnp.zeros((spare, channels), F32)], axis=0
        ).astype(BF16)
        for step in range(1, n_lon):
            remote(misc_s, misc_r.at[lon], mp_send, mp_recv, (lat, hop(step))).start()
        misc_r[lon] = misc_s[...]

    with scope("rswait"):
        drain(rs_r.at[pl.ds(0, n_lon - 1)], rs_recv)
    with scope("zsend"):
        rs_r[lon] = tot_b[lon]
        part = rs_r[0].astype(F32)
        for p in range(1, n_lon):
            part = part + rs_r[p].astype(F32)
        z_s[...] = part.astype(BF16)
        for step in range(1, n_lat):
            remote(z_s, z_r.at[lat], z_send, z_recv, (lax.rem(lat + step, n_lat), lon)).start()
        z_r[lat] = z_s[...]
        for turn in range(1, split):
            for step in range(first_part, n_lon):
                send_strip(side(turn), step)
        for step in range(1, n_lon):
            send_strip(group, step)
        main_o[group * n_lon + lon] = con_s[group, lon]

    with scope("miscz"):
        drain(misc_r.at[pl.ds(0, n_lon - 1)], mp_recv)
        part = misc_r[0].astype(F32)
        for p in range(1, n_lon):
            part = part + misc_r[p].astype(F32)
        misc_z[...] = part.astype(BF16)
        for step in range(1, n_lat):
            remote(misc_z, misc_o.at[lat], mz_send, mz_recv, (lax.rem(lat + step, n_lat), lon)).start()
        misc_o[lat] = misc_z[...]

    with scope("zwait"):
        drain(z_r.at[pl.ds(0, n_lat - 1)], z_recv)
    with scope("agsend"):
        part = z_r[0].astype(F32)
        for p in range(1, n_lat):
            part = part + z_r[p].astype(F32)
        fin_s[...] = part.astype(BF16)
        for step in range(1, n_lon):
            remote(fin_s, sums_o.at[lon], ag_send, ag_recv, (lat, hop(step))).start()
        sums_o[lon] = fin_s[...]

    with scope("mzwait"):
        drain(misc_o.at[pl.ds(0, n_lat - 1)], mz_recv)
    with scope("conwait"):
        drain(main_o.at[pl.ds(0, holders - 1)], con_recv)

        @pl.when(has_top)
        def _():
            drain(top_o, rim_recv.at[1])

        @pl.when(has_bot)
        def _():
            drain(bot_o, rim_recv.at[0])
    with scope("agwait"):
        drain(sums_o.at[pl.ds(0, n_lon - 1)], ag_recv)

    with scope("final"):
        drain(sbuf.at[pl.ds(0, peers - 1)], row_send)
        drain(cot_r.at[pl.ds(0, holders - 1)], cot_send)

        @pl.when(jnp.logical_and(lon == n_lon - 1, lat < n_lat - 1))
        def _():
            drain(top_o, edge_send)

        @pl.when(jnp.logical_and(lon == 0, lat > 0))
        def _():
            drain(top_o, edge_send)

        drain(main_o.at[pl.ds(0, holders - 1)], con_send)
        for h in range(split):
            @pl.when(tile_lat(h) > 0)
            def _():
                drain(con_e.at[0, 0], rim_send)

            @pl.when(tile_lat(h) < n_lat - 1)
            def _():
                drain(con_e.at[0, 0], rim_send)
        drain(rs_r.at[pl.ds(0, n_lon - 1)], rs_send)
        drain(misc_r.at[pl.ds(0, n_lon - 1)], mp_send)
        drain(z_r.at[pl.ds(0, n_lat - 1)], z_send)
        drain(misc_o.at[pl.ds(0, n_lat - 1)], mz_send)
        drain(sums_o.at[pl.ds(0, n_lon - 1)], ag_send)


def finish(
    n_lat, n_lon, split, own_rows, tile_cols, taps, hidden_size,
    main, top, bot, sums, misc, grid_o, gin_o, gb_o, gout_o, gk_o,
):
    piece, channels = sums.shape[1], sums.shape[2]
    here = iota((tile_cols, channels), 0)
    bodies = []
    for j in range(n_lon):
        value = main[j].astype(F32)
        for g in range(1, split):
            value = value + main[g * n_lon + j].astype(F32)
        ends = value[own_rows * tile_cols:own_rows * tile_cols + EDGE]
        rows = []
        for y in range(own_rows):
            body = value[y * tile_cols:(y + 1) * tile_cols]
            right = ends[(EDGE - 2 * y) % EDGE:(EDGE - 2 * y) % EDGE + 1]
            left = ends[EDGE - 1 - 2 * y:EDGE - 2 * y]
            for y_at, source in ((0, top), (own_rows - 1, bot)):
                if y == y_at:
                    extra = source[j].astype(F32)
                    for g in range(1, split):
                        extra = extra + source[g * n_lon + j].astype(F32)
                    body = body + extra[0:tile_cols]
                    right = right + extra[tile_cols:tile_cols + 1]
                    left = left + extra[tile_cols + EDGE - 1:tile_cols + EDGE]
            rows.append((body, right, left))
        bodies.append(rows)
    for j in range(n_lon):
        for y in range(own_rows):
            value = bodies[j][y][0]
            value = value + jnp.where(here == 0, bodies[(j - 1) % n_lon][y][1], 0.0)
            value = value + jnp.where(here == tile_cols - 1, bodies[(j + 1) % n_lon][y][2], 0.0)
            grid_o[y, j * tile_cols:(j + 1) * tile_cols, :] = value.astype(BF16)
    for p in range(n_lon):
        value = sums[p].astype(F32)
        start = p * piece
        for ref, low, high in ((gout_o, 0, hidden_size), (gin_o, hidden_size, n_lon * piece)):
            begin, end = max(start, low), min(start + piece, high)
            if begin < end:
                ref[begin - low:end - low, :] = value[begin - start:end - start]
    value = misc[0].astype(F32)
    for z in range(1, n_lat):
        value = value + misc[z].astype(F32)
    gb_o[...] = value[0:1]
    gk_o[...] = value[1:1 + taps]


def local(
    observations, owner_device, local_cell, valid_counts,
    weight_in, bias_in, weight_out, kernel_taps, cotangent,
):
    n_lat, n_lon = lax.axis_size("lat"), lax.axis_size("lon")
    n = n_lat * n_lon
    split = split_of(n_lat)
    obs_rows, feat = observations.shape
    hidden_size, channels = weight_out.shape
    own_rows, cols, _ = cotangent.shape
    tile_rows, tile_cols = own_rows * n_lon, cols // n_lon
    cells = tile_rows * tile_cols
    slots = round_up(2 * obs_rows // n, 16)
    batch = 4 if slots > 48 else 8
    piece = (hidden_size + feat) // n_lon
    taps = kernel_taps.shape[0]
    misc_rows = round_up(taps + 1, 16)
    peers = n // split
    holders = split * n_lon
    strip_rows = own_rows * tile_cols + EDGE
    wide = tile_cols + EDGE
    scale = 1.0 / math.sqrt(obs_rows * n)
    far = functools.partial(pltpu.with_memory_space_constraint, memory_space=pltpu.HBM)
    hbm = pl.BlockSpec(memory_space=pltpu.HBM)
    vmem = pl.BlockSpec(memory_space=pltpu.VMEM)
    dma = pltpu.SemaphoreType.DMA
    V = pltpu.VMEM
    found = pl.pallas_call(
        functools.partial(kernel, n_lat, n_lon, split, slots, batch, scale),
        out_shape=(
            V((holders, strip_rows, channels), BF16),
            V((holders, wide, channels), BF16),
            V((holders, wide, channels), BF16),
            V((n_lon, piece, channels), BF16),
            V((n_lat, misc_rows, channels), BF16),
        ),
        in_specs=[hbm, hbm, hbm, pl.BlockSpec(memory_space=pltpu.SMEM)] + [hbm] * 5,
        out_specs=(vmem,) * 5,
        scratch_shapes=[
            V((obs_rows, feat), BF16), V((1, obs_rows), jnp.int32), V((obs_rows // 128, 128), jnp.int32),
            V((feat, hidden_size), BF16), V((1, hidden_size), F32), V((hidden_size, channels), BF16),
            V((taps, channels), F32), V((own_rows, cols, channels), BF16),
            V((2 * n, 128), F32), V((1, obs_rows), jnp.int32),
            V((peers, split * slots + META, feat), BF16), V((peers, split * slots + META, feat), BF16),
            V((n_lon, strip_rows, channels), BF16), V((2, n_lon, wide, channels), BF16),
            V((holders, strip_rows, channels), BF16), V((split, wide, channels), BF16), V((split, wide, channels), BF16),
            V((split, tile_rows + 2, wide, channels), F32), V((cells, channels), F32), V((split, cells, channels), BF16),
            V((split, cells, channels), F32), V((split, 3, tile_rows + 4, wide, channels), F32),
            V((split, n_lon, strip_rows, channels), BF16), V((split, 2, wide, channels), BF16),
            V((taps, 8, channels), F32), V((hidden_size + feat, channels), F32), V((1, hidden_size), F32),
            V((n_lon, piece, channels), BF16), V((n_lon, piece, channels), BF16),
            V((piece, channels), BF16), V((n_lat, piece, channels), BF16), V((piece, channels), BF16),
            V((misc_rows, channels), BF16), V((n_lon, misc_rows, channels), BF16), V((misc_rows, channels), BF16),
            dma((8,)), dma, dma((peers // batch,)), dma, dma, dma, dma((split,)), dma((split,)),
            dma, dma, dma, dma((2,)), dma, dma, dma, dma, dma, dma,
            dma, dma, dma, dma,
        ],
        compiler_params=pltpu.CompilerParams(
            collective_id=0, has_side_effects=True, vmem_limit_bytes=48 * 1024 * 1024
        ),
    )(
        far(observations), far(owner_device.reshape(1, obs_rows)), far(local_cell.reshape(obs_rows // 128, 128)),
        valid_counts, far(weight_in), far(bias_in.reshape(1, hidden_size)), far(weight_out), far(kernel_taps),
        far(cotangent),
    )
    grid_out, grad_in, grad_bias, grad_out, grad_kernel = pl.pallas_call(
        functools.partial(finish, n_lat, n_lon, split, own_rows, tile_cols, taps, hidden_size),
        out_shape=(
            jax.ShapeDtypeStruct(cotangent.shape, BF16),
            jax.ShapeDtypeStruct((feat, hidden_size), F32),
            jax.ShapeDtypeStruct((1, hidden_size), F32),
            jax.ShapeDtypeStruct((hidden_size, channels), F32),
            jax.ShapeDtypeStruct((taps, channels), F32),
        ),
        in_specs=[vmem] * 5,
        out_specs=(vmem,) * 5,
    )(*[pltpu.with_memory_space_constraint(value, pltpu.VMEM) for value in found])
    return (grid_out, grad_in, grad_bias.reshape(hidden_size), grad_out, grad_kernel)


def solution(mesh):
    return jax.shard_map(
        local,
        mesh=mesh,
        in_specs=(
            P(("lat", "lon"), None),
            P(("lat", "lon"), None),
            P(("lat", "lon")),
            P(("lat", "lon")),
            P(),
            P(),
            P(),
            P(),
            P(("lat", "lon"), None, None),
        ),
        out_specs=(P(("lat", "lon"), None, None), P(), P(), P(), P()),
        check_vma=False,
    )
```

```python
import functools
import math

import jax
import jax.numpy as jnp
from jax import lax
from jax.experimental import pallas as pl
from jax.experimental.pallas import tpu as pltpu
from jax.sharding import PartitionSpec as P

MESH = pl.DeviceIdType.MESH
F32 = jnp.float32
BF16 = jnp.bfloat16
OFFSETS = [(a, b) for a in (-1, 0, 1) for b in (-1, 0, 1)]
CURVE = math.sqrt(2.0 / math.pi)
BEND = 0.044715
META = 8
EDGE = 8
EARLY = 2


def round_up(value, step):
    return -(-value // step) * step


def iota(shape, dim):
    return lax.broadcasted_iota(jnp.int32, shape, dim)


def dot(left, right, contract=((1,), (0,))):
    return lax.dot_general(left, right, (contract, ((), ())), preferred_element_type=F32)


def kernel(
    n_lat, n_lon, slots, batch, near_take, far_take, scale,
    obs_h, owner_h, cell_h, count, w_in_h, b_in_h, w_out_h, taps_h, cot_h,
    main_o, top_o, bot_o, sums_o, misc_o,
    obs, owner, cell, w_in, b_in, w_out, taps, cot,
    meta, slot_row, sbuf, rbuf, cot_s, cot_e, cot_r, cot_top, cot_bot, c32, adj_f, adj_b,
    dep, moved, con_s, con_e, gka, total, bias, tot_b, rs_r, z_s, z_r, fin_s, misc_s, misc_r, misc_z,
    in_sem, row_send, row_recv, cot_send, cot_recv, edge_send, top_recv, bot_recv,
    con_send, con_recv, rim_send, rim_recv, rs_send, rs_recv, z_send, z_recv, ag_send, ag_recv,
    mp_send, mp_recv, mz_send, mz_recv,
):
    n = n_lat * n_lon
    lat, lon = lax.axis_index("lat"), lax.axis_index("lon")
    me = lat * n_lon + lon
    deep = n_lat // 2
    peers = deep * n_lon
    group, level = lat // deep, lax.rem(lat, deep)
    dense = lax.rem(lon, 2) == 0
    far_lat = lax.rem(lat + deep, n_lat)
    tile_lat = (lat, far_lat)
    obs_rows, feat = obs.shape
    own_rows, cols, channels = cot.shape
    tile_rows, tile_cols = own_rows * n_lon, cols // n_lon
    cells = tile_rows * tile_cols
    wide = tile_cols + EDGE
    hidden_size = w_in.shape[1]
    piece = tot_b.shape[1]
    holders = n_lon + n_lon // 2
    scope = jax.named_scope

    def wrap(value, size):
        return jnp.where(value >= size, value - size, value)

    def hop(step):
        return wrap(lon + step, n_lon)

    def seat(off):
        return wrap(level + lax.rem(off, deep), deep), wrap(lon + off // deep, n_lon)

    def near(off):
        to_level, to_lon = seat(off)
        to_lat = group * deep + to_level
        return (to_lat, to_lon), to_lat * n_lon + to_lon

    def far(off):
        to_level, to_lon = seat(off)
        to_lat = (1 - group) * deep + to_level
        stand_in = lax.rem(to_lon, 2) == 0
        return (jnp.where(stand_in, group * deep + to_level, to_lat), to_lon), to_lat * n_lon + to_lon

    def remote(src, dst, send, recv, device):
        return pltpu.make_async_remote_copy(
            src_ref=src, dst_ref=dst, send_sem=send, recv_sem=recv,
            device_id=device, device_id_type=MESH,
        )

    def drain(ref, sem):
        pltpu.make_async_copy(ref, ref, sem).wait()

    pairs = [
        (owner_h, owner), (cell_h, cell), (obs_h, obs), (cot_h, cot),
        (w_in_h, w_in), (b_in_h, b_in), (w_out_h, w_out), (taps_h, taps),
    ]
    fetches = [pltpu.make_async_copy(src, dst, in_sem.at[i]) for i, (src, dst) in enumerate(pairs)]
    for fetch in fetches:
        fetch.start()

    barrier = pltpu.get_barrier_semaphore()

    def signal(to_lat, to_lon):
        pl.semaphore_signal(barrier, inc=1, device_id=(to_lat, to_lon), device_id_type=MESH)

    def greet(turn, carry):
        to_lat = wrap(lat + turn, n_lat)
        for step in range(n_lon):
            signal(to_lat, hop(step))
        return carry

    with scope("greet"):
        lax.fori_loop(1, n_lat, greet, 0)
        for step in range(1, n_lon):
            signal(lat, hop(step))

    with scope("zero"):
        for s in range(2):
            @pl.when(tile_lat[s] == 0)
            def _(s=s):
                cot_top[s] = jnp.zeros((wide, channels), BF16)

            @pl.when(tile_lat[s] == n_lat - 1)
            def _(s=s):
                cot_bot[s] = jnp.zeros((wide, channels), BF16)

        has_top = jnp.logical_and(lon == 0, lat > 0)
        has_bot = jnp.logical_and(lon == n_lon - 1, lat < n_lat - 1)

        @pl.when(jnp.logical_not(has_top))
        def _():
            top_o[...] = jnp.zeros_like(top_o)

        @pl.when(jnp.logical_not(has_bot))
        def _():
            bot_o[...] = jnp.zeros_like(bot_o)

    with scope("meta"):
        fetches[0].wait()
        own_row = owner[...]
        match = (own_row == iota((n, obs_rows), 0)).astype(F32)
        block = 256 if obs_rows % 256 == 0 else 128
        upper = (iota((block, block), 0) < iota((block, block), 1)).astype(F32).astype(BF16)
        carry = jnp.zeros((n, 1), F32)
        ranks = []
        for start in range(0, obs_rows, block):
            part = match[:, start:start + block]
            before = dot(part.astype(BF16), upper) + carry
            ranks.append(jnp.sum(before * part, axis=0, keepdims=True))
            carry = carry + jnp.sum(part, axis=1, keepdims=True)
        rank = jnp.concatenate(ranks, axis=1).astype(jnp.int32)
        slot_row[...] = own_row * slots + rank
        fetches[1].wait()
        lane = iota((1, obs_rows), 1)
        cells_row = jnp.concatenate([cell[i:i + 1, :] for i in range(obs_rows // 128)], axis=1)
        code = jnp.where(lane < count[0], cells_row + 1, 0)
        high = (code // 128).astype(F32)
        low = lax.rem(code, 128).astype(F32)
        coded = jnp.concatenate([match * high, match * low], axis=0).astype(BF16)
        by_rank = (rank == iota((128, obs_rows), 0)).astype(F32).astype(BF16)
        meta[...] = dot(coded, by_rank, ((1,), (1,)))
        fetches[2].wait()

    def prepare(first, where):
        base = 0 if where is near else peers
        ids = slot_row[...]
        picks = []
        targets = []
        for u in range(batch):
            _, target = where(first + u)
            targets.append(target)
            rel = jnp.clip(ids - target * slots, -1, slots).astype(F32)
            rel = jnp.broadcast_to(rel, (16, obs_rows)).astype(BF16)
            for at in range(0, slots, 16):
                line = (iota((16, obs_rows), 0) + at).astype(F32).astype(BF16)
                picks.append(jnp.where(rel == line, jnp.ones_like(line), jnp.zeros_like(line)))
        rows = dot(jnp.concatenate(picks, axis=0), obs[...]).astype(BF16)
        line = iota((META, 128), 0)
        for u in range(batch):
            at = base + first + u
            sbuf[at, 0:slots, :] = rows[u * slots:(u + 1) * slots]
            tail = jnp.where(
                line == 0, meta[pl.ds(targets[u], 1), :],
                jnp.where(line == 1, meta[pl.ds(n + targets[u], 1), :], 0.0),
            )
            sbuf[at, slots:slots + META, :] = tail.astype(BF16)

    near_takes, far_takes = peers // near_take, peers // far_take

    def ship_near(off):
        to, _ = near(off)
        remote(sbuf.at[off], rbuf.at[off], row_send, row_recv.at[off // near_take], to).start()

    def ship_far(off):
        to, _ = far(off)
        remote(
            sbuf.at[peers + off], rbuf.at[peers + off], row_send, row_recv.at[near_takes + off // far_take], to
        ).start()

    def prepare_near(p, carry):
        prepare(p * batch, near)
        return carry

    def prepare_far(p, carry):
        prepare(p * batch, far)
        return carry

    rounds = peers // batch
    with scope("prep0"):
        lax.fori_loop(0, min(EARLY, rounds), prepare_near, 0)

    with scope("cotprep"):
        fetches[3].wait()
        rim = iota((EDGE, channels), 0)
        rows_f = [cot[y].astype(F32) for y in range(own_rows)]
        for j in range(n_lon):
            start, stop = j * tile_cols, (j + 1) * tile_cols
            after, ahead = stop % cols, (start - EDGE) % cols
            mixed = jnp.zeros((EDGE, channels), F32)
            for y in range(own_rows):
                row = rows_f[y]
                ends = jnp.where(
                    rim == 0, row[after:after + EDGE],
                    jnp.where(rim == EDGE - 1, row[ahead:ahead + EDGE], 0.0),
                )
                cot_s[j, y * tile_cols:(y + 1) * tile_cols, :] = cot[y, start:stop, :]
                mixed = mixed + (pltpu.roll(ends, EDGE - 2 * y, 0) if y else ends)
                if y == 0:
                    cot_e[0, j, 0:tile_cols, :] = cot[y, start:stop, :]
                    cot_e[0, j, tile_cols:wide, :] = ends.astype(BF16)
                if y == own_rows - 1:
                    cot_e[1, j, 0:tile_cols, :] = cot[y, start:stop, :]
                    cot_e[1, j, tile_cols:wide, :] = ends.astype(BF16)
            cot_s[j, own_rows * tile_cols:own_rows * tile_cols + EDGE, :] = mixed.astype(BF16)

    with scope("barw"):
        pl.semaphore_wait(barrier, n - 1)

    with scope("ship"):
        def send_edges(e, to_tile, dst, sem):
            far_tile = lax.rem(to_tile + deep, n_lat)
            for j in range(n_lon):
                remote(cot_e.at[e, j], dst.at[0], edge_send, sem.at[0], (to_tile, j)).start()
                if j % 2 == 0:
                    remote(cot_e.at[e, j], dst.at[1], edge_send, sem.at[1], (far_tile, j)).start()

        @pl.when(jnp.logical_and(lon == n_lon - 1, lat < n_lat - 1))
        def _():
            send_edges(1, lat + 1, cot_top, top_recv)

        @pl.when(jnp.logical_and(lon == 0, lat > 0))
        def _():
            send_edges(0, lat - 1, cot_bot, bot_recv)

        for step in range(1, n_lon):
            remote(cot_s.at[hop(step)], cot_r.at[lon], cot_send, cot_recv.at[0], (lat, hop(step))).start()
        cot_r[lon] = cot_s[lon]
        for step in range(n_lon // 2):
            other = 2 * wrap(lon // 2 + step, n_lon // 2)
            remote(
                cot_s.at[other], cot_r.at[n_lon + lon], cot_send, cot_recv.at[1], (far_lat, other)
            ).start()


        def ship_first(p):
            @pl.when(p == 0)
            def _():
                pltpu.make_async_copy(sbuf.at[0], rbuf.at[0], row_recv.at[0]).start()

            @pl.when(p > 0)
            def _():
                ship_near(p * batch)

        def ship_near_batch(p, carry):
            ship_first(p)
            for u in range(1, batch):
                ship_near(p * batch + u)
            return carry

        lax.fori_loop(0, min(EARLY, rounds), ship_near_batch, 0)

    with scope("prep1"):
        if EARLY < rounds:
            lax.fori_loop(EARLY, rounds, lambda p, c: ship_near_batch(p, prepare_near(p, c)), 0)

    with scope("prep2"):
        def far_round(p, carry):
            prepare_far(p, carry)
            own = jnp.logical_and(p == 0, dense)

            @pl.when(own)
            def _():
                pltpu.make_async_copy(sbuf.at[peers], rbuf.at[peers], row_recv.at[near_takes]).start()

            @pl.when(jnp.logical_not(own))
            def _():
                ship_far(p * batch)

            for u in range(1, batch):
                ship_far(p * batch + u)
            return carry

        lax.fori_loop(0, rounds, far_round, 0)

    with scope("clear"):
        for s in range(2):
            for b in range(3):
                for i in (0, 1, tile_rows + 2, tile_rows + 3):
                    moved[s, b, i] = jnp.zeros((wide, channels), F32)
        dep[...] = jnp.zeros_like(dep)
        total[...] = jnp.zeros_like(total)
        bias[...] = jnp.zeros_like(bias)
        gka[...] = jnp.zeros_like(gka)

    def cot_wait(s):
        if s == 0:
            drain(cot_r.at[pl.ds(0, n_lon - 1)], cot_recv.at[0])
        else:
            drain(cot_r.at[pl.ds(0, n_lon)], cot_recv.at[1])

        @pl.when(tile_lat[s] > 0)
        def _():
            drain(cot_top.at[s], top_recv.at[s])

        @pl.when(tile_lat[s] < n_lat - 1)
        def _():
            drain(cot_bot.at[s], bot_recv.at[s])

    half = channels // 2
    for fetch in fetches[4:]:
        fetch.wait()
    tap = taps[...]

    def adjoint(h):
        c32[h, 0] = cot_top[h].astype(F32)
        c32[h, tile_rows + 1] = cot_bot[h].astype(F32)

        def widen(j, carry):
            at = h * n_lon + j
            ends = cot_r[at, own_rows * tile_cols:own_rows * tile_cols + EDGE, :].astype(F32)
            for r in range(own_rows):
                m = j * own_rows + r + 1
                c32[h, m, 0:tile_cols, :] = cot_r[at, r * tile_cols:(r + 1) * tile_cols, :].astype(F32)
                c32[h, m, tile_cols:wide, :] = pltpu.roll(ends, 2 * r, 0) if r else ends
            return carry

        lax.fori_loop(0, n_lon, widen, 0)

        def adjoin(m, carry):
            for c in range(0, channels, half):
                acc = jnp.zeros((tile_cols, half), F32)
                for a in (-1, 0, 1):
                    row = c32[h, m + 1 - a, :, c:c + half]
                    for b in (-1, 0, 1):
                        k = 3 * (a + 1) + b + 1
                        turned = pltpu.roll(row, b % wide, 0) if b else row
                        acc = acc + tap[k:k + 1, c:c + half] * turned[0:tile_cols]
                adj_f[pl.ds(pl.multiple_of(m * tile_cols, 8), tile_cols), c:c + half] = scale * acc
            return carry

        lax.fori_loop(0, tile_rows, adjoin, 0)
        adj_b[h] = adj_f[...].astype(BF16)

    def take(s, first, size, sem):
        with scope("rowwait"):
            drain(rbuf.at[pl.ds(first, size)], sem)
        rows = jnp.concatenate([rbuf[first + q, 0:slots, :] for q in range(size)], axis=0)
        codes = []
        for q in range(size):
            tail = rbuf[first + q, slots:slots + META, :].astype(F32)
            codes.append((128.0 * tail[0:1] + tail[1:2])[:, 0:slots])
        codes = jnp.concatenate(codes, axis=1).astype(jnp.int32)
        pick = (codes == iota((cells, size * slots), 0) + 1).astype(F32).astype(BF16)
        upstream = dot(pick, adj_b[s], ((0,), (0,))).astype(BF16)
        x = dot(rows, w_in[...]) + b_in[...]
        square = x * x
        t_val = jnp.tanh(x * (CURVE + (CURVE * BEND) * square))
        upper_half = 0.5 + 0.5 * t_val
        lower_half = 0.5 - 0.5 * t_val
        active = x * upper_half
        hidden = active.astype(BF16)
        slope = upper_half + (active * lower_half) * (2.0 * CURVE + (6.0 * CURVE * BEND) * square)
        encoded = dot(hidden, w_out[...]).astype(BF16)
        dep[s] += dot(pick, encoded)
        back = dot(upstream, w_out[...], ((1,), (1,)))
        pre = (back * slope).astype(BF16)
        total[0:hidden_size, :] += dot(hidden, upstream, ((0,), (0,)))
        total[hidden_size:hidden_size + feat, :] += dot(rows, pre, ((0,), (0,)))
        bias[...] += jnp.sum(pre.astype(F32), axis=0, keepdims=True)

    with scope("cotwaitA"):
        cot_wait(0)
    with scope("adjointA"):
        adjoint(0)

    def take_near(t, carry):
        take(0, t * near_take, near_take, row_recv.at[t])
        return carry

    def take_far(t, carry):
        take(1, peers + t * far_take, far_take, row_recv.at[near_takes + t])
        return carry

    def take_pair(t, carry):
        take_near(t + lead, carry)
        take_far(t, carry)
        return carry

    lead = rounds // 2
    with scope("takeA"):
        lax.fori_loop(0, lead, take_near, 0)
    with scope("adjointB"):
        @pl.when(dense)
        def _():
            with scope("cotwaitB"):
                cot_wait(1)
            adjoint(1)

        @pl.when(jnp.logical_not(dense))
        def _():
            adj_b[1] = adj_b[0]

    with scope("takeAB"):
        lax.fori_loop(0, rounds - lead, take_pair, 0)
    with scope("takeB"):
        lax.fori_loop(rounds - lead, rounds, take_far, 0)

    with scope("rssend"):
        for p in range(n_lon):
            tot_b[p] = total[p * piece:(p + 1) * piece, :].astype(BF16)
        for step in range(1, n_lon):
            remote(tot_b.at[hop(step)], rs_r.at[lon], rs_send, rs_recv, (lat, hop(step))).start()

    def spread(h):
        def turn_row(m, carry):
            row = dep[h, pl.ds(pl.multiple_of(m * tile_cols, 8), tile_cols), :]
            row = jnp.concatenate([row, jnp.zeros((EDGE, channels), F32)], axis=0)
            moved[h, 0, m + 2] = pltpu.roll(row, 1, 0)
            moved[h, 1, m + 2] = row
            moved[h, 2, m + 2] = pltpu.roll(row, wide - 1, 0)
            return carry

        lax.fori_loop(0, tile_rows, turn_row, 0)

        def out_row(i, c):
            acc = jnp.zeros((wide, half), F32)
            seen = c32[h, i, :, c:c + half]
            for a in (-1, 0, 1):
                for b in (-1, 0, 1):
                    k = 3 * (a + 1) + b + 1
                    value = moved[h, b + 1, i + 1 + a, :, c:c + half]
                    acc = acc + tap[k:k + 1, c:c + half] * value
                    prod = seen * value
                    folded = prod[0:8]
                    for at in range(8, wide, 8):
                        folded = folded + prod[at:at + 8]
                    gka[k, :, c:c + half] += folded
            return acc

        def strip(j, carry):
            for c in range(0, channels, half):
                mixed = jnp.zeros((EDGE, half), F32)
                for r in range(own_rows):
                    acc = out_row(j * own_rows + r + 1, c)
                    con_s[h, j, r * tile_cols:(r + 1) * tile_cols, c:c + half] = acc[0:tile_cols].astype(BF16)
                    ends = acc[tile_cols:wide]
                    mixed = mixed + (pltpu.roll(ends, EDGE - 2 * r, 0) if r else ends)
                con_s[h, j, own_rows * tile_cols:own_rows * tile_cols + EDGE, c:c + half] = mixed.astype(BF16)
            return carry

        for e, i in ((0, 0), (1, tile_rows + 1)):
            for c in range(0, channels, half):
                con_e[h, e, :, c:c + half] = out_row(i, c).astype(BF16)
        lax.fori_loop(0, n_lon, strip, 0)

    def send_strip(h, step):
        where = lon if h == 0 else n_lon + lon // 2
        remote(
            con_s.at[h, hop(step)], main_o.at[where], con_send, con_recv, (tile_lat[h], hop(step))
        ).start()

    def rim_copy(h, e):
        where = lon if h == 0 else n_lon + lon // 2
        if e == 0:
            return remote(con_e.at[h, 0], bot_o.at[where], rim_send, rim_recv.at[0], (tile_lat[h] - 1, n_lon - 1))
        return remote(con_e.at[h, 1], top_o.at[where], rim_send, rim_recv.at[1], (tile_lat[h] + 1, 0))

    def rims(h, act):
        @pl.when(tile_lat[h] > 0)
        def _():
            act(rim_copy(h, 0))

        @pl.when(tile_lat[h] < n_lat - 1)
        def _():
            act(rim_copy(h, 1))

    first_part = n_lon // 2
    with scope("spread"):
        @pl.when(dense)
        def _():
            spread(1)
            rims(1, lambda copy: copy.start())
            for step in range(first_part):
                send_strip(1, step)

        @pl.when(jnp.logical_not(dense))
        def _():
            dep[0] += dep[1]

        spread(0)
        rims(0, lambda copy: copy.start())

    with scope("misc"):
        grads = [jnp.sum(gka[k], axis=0, keepdims=True) * scale for k in range(len(OFFSETS))]
        spare = misc_s.shape[0] - len(OFFSETS) - 1
        misc_s[...] = jnp.concatenate(
            [bias[...]] + grads + [jnp.zeros((spare, channels), F32)], axis=0
        ).astype(BF16)
        for step in range(1, n_lon):
            remote(misc_s, misc_r.at[lon], mp_send, mp_recv, (lat, hop(step))).start()
        misc_r[lon] = misc_s[...]

    with scope("rswait"):
        drain(rs_r.at[pl.ds(0, n_lon - 1)], rs_recv)
    with scope("zsend"):
        rs_r[lon] = tot_b[lon]
        part = rs_r[0].astype(F32)
        for p in range(1, n_lon):
            part = part + rs_r[p].astype(F32)
        z_s[...] = part.astype(BF16)
        for step in range(1, n_lat):
            remote(z_s, z_r.at[lat], z_send, z_recv, (wrap(lat + step, n_lat), lon)).start()
        z_r[lat] = z_s[...]

        @pl.when(dense)
        def _():
            for step in range(first_part, n_lon):
                send_strip(1, step)

        for step in range(1, n_lon):
            send_strip(0, step)
        main_o[lon] = con_s[0, lon]

    with scope("miscz"):
        drain(misc_r.at[pl.ds(0, n_lon - 1)], mp_recv)
        part = misc_r[0].astype(F32)
        for p in range(1, n_lon):
            part = part + misc_r[p].astype(F32)
        misc_z[...] = part.astype(BF16)
        for step in range(1, n_lat):
            remote(misc_z, misc_o.at[lat], mz_send, mz_recv, (wrap(lat + step, n_lat), lon)).start()
        misc_o[lat] = misc_z[...]

    with scope("zwait"):
        drain(z_r.at[pl.ds(0, n_lat - 1)], z_recv)
    with scope("agsend"):
        part = z_r[0].astype(F32)
        for p in range(1, n_lat):
            part = part + z_r[p].astype(F32)
        fin_s[...] = part.astype(BF16)
        for step in range(1, n_lon):
            remote(fin_s, sums_o.at[lon], ag_send, ag_recv, (lat, hop(step))).start()
        sums_o[lon] = fin_s[...]

    with scope("mzwait"):
        drain(misc_o.at[pl.ds(0, n_lat - 1)], mz_recv)
    with scope("conwait"):
        drain(main_o.at[pl.ds(0, holders - 1)], con_recv)

        @pl.when(has_top)
        def _():
            drain(top_o, rim_recv.at[1])

        @pl.when(has_bot)
        def _():
            drain(bot_o, rim_recv.at[0])
    with scope("agwait"):
        drain(sums_o.at[pl.ds(0, n_lon - 1)], ag_recv)

    with scope("final"):
        drain(sbuf.at[pl.ds(0, 2 * peers - 2)], row_send)

        @pl.when(jnp.logical_not(dense))
        def _():
            drain(sbuf.at[0], row_send)

        drain(cot_r.at[pl.ds(0, holders - 1)], cot_send)

        @pl.when(jnp.logical_and(lon == n_lon - 1, lat < n_lat - 1))
        def _():
            drain(top_o, edge_send)

        @pl.when(jnp.logical_and(lon == 0, lat > 0))
        def _():
            drain(top_o, edge_send)

        drain(main_o.at[pl.ds(0, n_lon - 1)], con_send)
        rims(0, lambda copy: copy.wait_send())

        @pl.when(dense)
        def _():
            drain(main_o.at[pl.ds(0, n_lon)], con_send)
            rims(1, lambda copy: copy.wait_send())

        drain(rs_r.at[pl.ds(0, n_lon - 1)], rs_send)
        drain(misc_r.at[pl.ds(0, n_lon - 1)], mp_send)
        drain(z_r.at[pl.ds(0, n_lat - 1)], z_send)
        drain(misc_o.at[pl.ds(0, n_lat - 1)], mz_send)
        drain(sums_o.at[pl.ds(0, n_lon - 1)], ag_send)


def finish(
    n_lat, n_lon, own_rows, tile_cols, taps, hidden_size,
    main, top, bot, sums, misc, grid_o, gin_o, gb_o, gout_o, gk_o,
):
    piece, channels = sums.shape[1], sums.shape[2]
    here = iota((tile_cols, channels), 0)

    def both(ref, j):
        value = ref[j].astype(F32)
        return value if j % 2 else value + ref[n_lon + j // 2].astype(F32)

    bodies = []
    for j in range(n_lon):
        value = both(main, j)
        ends = value[own_rows * tile_cols:own_rows * tile_cols + EDGE]
        rows = []
        for y in range(own_rows):
            body = value[y * tile_cols:(y + 1) * tile_cols]
            right = ends[(EDGE - 2 * y) % EDGE:(EDGE - 2 * y) % EDGE + 1]
            left = ends[EDGE - 1 - 2 * y:EDGE - 2 * y]
            for y_at, source in ((0, top), (own_rows - 1, bot)):
                if y == y_at:
                    extra = both(source, j)
                    body = body + extra[0:tile_cols]
                    right = right + extra[tile_cols:tile_cols + 1]
                    left = left + extra[tile_cols + EDGE - 1:tile_cols + EDGE]
            rows.append((body, right, left))
        bodies.append(rows)
    for j in range(n_lon):
        for y in range(own_rows):
            value = bodies[j][y][0]
            value = value + jnp.where(here == 0, bodies[(j - 1) % n_lon][y][1], 0.0)
            value = value + jnp.where(here == tile_cols - 1, bodies[(j + 1) % n_lon][y][2], 0.0)
            grid_o[y, j * tile_cols:(j + 1) * tile_cols, :] = value.astype(BF16)
    for p in range(n_lon):
        value = sums[p].astype(F32)
        start = p * piece
        for ref, low, high in ((gout_o, 0, hidden_size), (gin_o, hidden_size, n_lon * piece)):
            begin, end = max(start, low), min(start + piece, high)
            if begin < end:
                ref[begin - low:end - low, :] = value[begin - start:end - start]
    value = misc[0].astype(F32)
    for z in range(1, n_lat):
        value = value + misc[z].astype(F32)
    gb_o[...] = value[0:1]
    gk_o[...] = value[1:1 + taps]


def local(
    observations, owner_device, local_cell, valid_counts,
    weight_in, bias_in, weight_out, kernel_taps, cotangent,
):
    n_lat, n_lon = lax.axis_size("lat"), lax.axis_size("lon")
    n = n_lat * n_lon
    obs_rows, feat = observations.shape
    hidden_size, channels = weight_out.shape
    own_rows, cols, _ = cotangent.shape
    tile_rows, tile_cols = own_rows * n_lon, cols // n_lon
    cells = tile_rows * tile_cols
    slots = round_up(2 * obs_rows // n, 16)
    batch = 4 if slots > 48 else 8
    near_take, far_take = batch, batch
    piece = (hidden_size + feat) // n_lon
    taps = kernel_taps.shape[0]
    misc_rows = round_up(taps + 1, 16)
    peers = n // 2
    holders = n_lon + n_lon // 2
    strip_rows = own_rows * tile_cols + EDGE
    wide = tile_cols + EDGE
    scale = 1.0 / math.sqrt(obs_rows * n)
    far = functools.partial(pltpu.with_memory_space_constraint, memory_space=pltpu.HBM)
    hbm = pl.BlockSpec(memory_space=pltpu.HBM)
    vmem = pl.BlockSpec(memory_space=pltpu.VMEM)
    dma = pltpu.SemaphoreType.DMA
    V = pltpu.VMEM
    found = pl.pallas_call(
        functools.partial(kernel, n_lat, n_lon, slots, batch, near_take, far_take, scale),
        out_shape=(
            V((holders, strip_rows, channels), BF16),
            V((holders, wide, channels), BF16),
            V((holders, wide, channels), BF16),
            V((n_lon, piece, channels), BF16),
            V((n_lat, misc_rows, channels), BF16),
        ),
        in_specs=[hbm, hbm, hbm, pl.BlockSpec(memory_space=pltpu.SMEM)] + [hbm] * 5,
        out_specs=(vmem,) * 5,
        scratch_shapes=[
            V((obs_rows, feat), BF16), V((1, obs_rows), jnp.int32), V((obs_rows // 128, 128), jnp.int32),
            V((feat, hidden_size), BF16), V((1, hidden_size), F32), V((hidden_size, channels), BF16),
            V((taps, channels), F32), V((own_rows, cols, channels), BF16),
            V((2 * n, 128), F32), V((1, obs_rows), jnp.int32),
            V((n, slots + META, feat), BF16), V((n, slots + META, feat), BF16),
            V((n_lon, strip_rows, channels), BF16), V((2, n_lon, wide, channels), BF16),
            V((2 * n_lon, strip_rows, channels), BF16), V((2, wide, channels), BF16), V((2, wide, channels), BF16),
            V((2, tile_rows + 2, wide, channels), F32), V((cells, channels), F32), V((2, cells, channels), BF16),
            V((2, cells, channels), F32), V((2, 3, tile_rows + 4, wide, channels), F32),
            V((2, n_lon, strip_rows, channels), BF16), V((2, 2, wide, channels), BF16),
            V((taps, 8, channels), F32), V((hidden_size + feat, channels), F32), V((1, hidden_size), F32),
            V((n_lon, piece, channels), BF16), V((n_lon, piece, channels), BF16),
            V((piece, channels), BF16), V((n_lat, piece, channels), BF16), V((piece, channels), BF16),
            V((misc_rows, channels), BF16), V((n_lon, misc_rows, channels), BF16), V((misc_rows, channels), BF16),
            dma((8,)), dma, dma((peers // near_take + peers // far_take,)), dma, dma((2,)), dma, dma((2,)), dma((2,)),
            dma, dma, dma, dma((2,)), dma, dma, dma, dma, dma, dma,
            dma, dma, dma, dma,
        ],
        compiler_params=pltpu.CompilerParams(
            collective_id=0, has_side_effects=True, vmem_limit_bytes=48 * 1024 * 1024
        ),
    )(
        far(observations), far(owner_device.reshape(1, obs_rows)), far(local_cell.reshape(obs_rows // 128, 128)),
        valid_counts, far(weight_in), far(bias_in.reshape(1, hidden_size)), far(weight_out), far(kernel_taps),
        far(cotangent),
    )
    grid_out, grad_in, grad_bias, grad_out, grad_kernel = pl.pallas_call(
        functools.partial(finish, n_lat, n_lon, own_rows, tile_cols, taps, hidden_size),
        out_shape=(
            jax.ShapeDtypeStruct(cotangent.shape, BF16),
            jax.ShapeDtypeStruct((feat, hidden_size), F32),
            jax.ShapeDtypeStruct((1, hidden_size), F32),
            jax.ShapeDtypeStruct((hidden_size, channels), F32),
            jax.ShapeDtypeStruct((taps, channels), F32),
        ),
        in_specs=[vmem] * 5,
        out_specs=(vmem,) * 5,
    )(*[pltpu.with_memory_space_constraint(value, pltpu.VMEM) for value in found])
    return (grid_out, grad_in, grad_bias.reshape(hidden_size), grad_out, grad_kernel)


def solution(mesh):
    return jax.shard_map(
        local,
        mesh=mesh,
        in_specs=(
            P(("lat", "lon"), None),
            P(("lat", "lon"), None),
            P(("lat", "lon")),
            P(("lat", "lon")),
            P(),
            P(),
            P(),
            P(),
            P(("lat", "lon"), None, None),
        ),
        out_specs=(P(("lat", "lon"), None, None), P(), P(), P(), P()),
        check_vma=False,
    )
```

```python
import functools
import math

import jax
import jax.numpy as jnp
from jax import lax
from jax.experimental import pallas as pl
from jax.experimental.pallas import tpu as pltpu
from jax.sharding import PartitionSpec as P

MESH = pl.DeviceIdType.MESH
F32 = jnp.float32
BF16 = jnp.bfloat16
OFFSETS = [(a, b) for a in (-1, 0, 1) for b in (-1, 0, 1)]
CURVE = math.sqrt(2.0 / math.pi)
BEND = 0.044715
EDGE = 8
EARLY = 2
SEND = (("n", 0), ("n", 1), ("n", 2), ("n", 3), ("f", 0), ("f", 1), ("f", 2), ("f", 3))
LATE = 2


def round_up(value, step):
    return -(-value // step) * step


def iota(shape, dim):
    return lax.broadcasted_iota(jnp.int32, shape, dim)


def dot(left, right, contract=((1,), (0,))):
    return lax.dot_general(left, right, (contract, ((), ())), preferred_element_type=F32)


def kernel(
    n_lat, n_lon, slots, batch, scale,
    obs_h, owner_h, cell_h, count, w_in_h, b_in_h, w_out_h, taps_h, cot_h,
    grid_o, gin_o, gb_o, gout_o, gk_o,
    obs, owner, cell, w_in, b_in, w_out, taps, cot,
    main_o, top_o, bot_o, sums_o, misc_o,
    meta, meta_r, slot_row, sbuf, rbuf, cot_s, cot_e, cot_r, cot_top, cot_bot, c32, adj_f, adj_b,
    dep, moved, con_s, con_e, gka, total, bias, tot_b, rs_r, z_s, z_r, fin_s, misc_s, misc_r, misc_z,
    in_sem, meta_send, meta_recv, row_send, row_recv, cot_send, cot_recv, edge_send, top_recv, bot_recv,
    con_send, con_recv, rim_send, rim_recv, rs_send, rs_recv, z_send, z_recv, ag_send, ag_recv,
    mp_send, mp_recv, mz_send, mz_recv,
):
    n = n_lat * n_lon
    lat, lon = lax.axis_index("lat"), lax.axis_index("lon")
    me = lat * n_lon + lon
    deep = n_lat // 2
    peers = deep * n_lon
    group, level = lat // deep, lax.rem(lat, deep)
    dense = lax.rem(lon, 2) == 0
    far_lat = lax.rem(lat + deep, n_lat)
    tile_lat = (lat, far_lat)
    obs_rows, feat = obs.shape
    own_rows, cols, channels = cot.shape
    tile_rows, tile_cols = own_rows * n_lon, cols // n_lon
    cells = tile_rows * tile_cols
    wide = tile_cols + EDGE
    hidden_size = w_in.shape[1]
    piece = tot_b.shape[1]
    holders = n_lon + n_lon // 2
    scope = jax.named_scope

    def wrap(value, size):
        return jnp.where(value >= size, value - size, value)

    def hop(step):
        return wrap(lon + step, n_lon)

    def seat(off):
        return wrap(level + off // n_lon, deep), wrap(lon + lax.rem(off, n_lon), n_lon)

    def near(off):
        to_level, to_lon = seat(off)
        to_lat = group * deep + to_level
        return (to_lat, to_lon), to_lat * n_lon + to_lon

    def far(off):
        to_level, to_lon = seat(off)
        to_lat = (1 - group) * deep + to_level
        stand_in = lax.rem(to_lon, 2) == 0
        return (jnp.where(stand_in, group * deep + to_level, to_lat), to_lon), to_lat * n_lon + to_lon

    def remote(src, dst, send, recv, device):
        return pltpu.make_async_remote_copy(
            src_ref=src, dst_ref=dst, send_sem=send, recv_sem=recv,
            device_id=device, device_id_type=MESH,
        )

    def drain(ref, sem):
        pltpu.make_async_copy(ref, ref, sem).wait()

    pairs = [
        (owner_h, owner), (cell_h, cell), (obs_h, obs), (cot_h, cot),
        (w_in_h, w_in), (b_in_h, b_in), (w_out_h, w_out), (taps_h, taps),
    ]
    fetches = [pltpu.make_async_copy(src, dst, in_sem.at[i]) for i, (src, dst) in enumerate(pairs)]
    for fetch in fetches:
        fetch.start()

    barrier = pltpu.get_barrier_semaphore()

    def signal(to_lat, to_lon):
        pl.semaphore_signal(barrier, inc=1, device_id=(to_lat, to_lon), device_id_type=MESH)

    def greet(turn, carry):
        to_lat = wrap(lat + turn, n_lat)
        for step in range(n_lon):
            signal(to_lat, hop(step))
        return carry

    with scope("greet"):
        lax.fori_loop(1, n_lat, greet, 0)
        for step in range(1, n_lon):
            signal(lat, hop(step))

    with scope("zero"):
        for s in range(2):
            @pl.when(tile_lat[s] == 0)
            def _(s=s):
                cot_top[s] = jnp.zeros((wide, channels), BF16)

            @pl.when(tile_lat[s] == n_lat - 1)
            def _(s=s):
                cot_bot[s] = jnp.zeros((wide, channels), BF16)

        has_top = jnp.logical_and(lon == 0, lat > 0)
        has_bot = jnp.logical_and(lon == n_lon - 1, lat < n_lat - 1)

        @pl.when(jnp.logical_not(has_top))
        def _():
            top_o[...] = jnp.zeros_like(top_o)

        @pl.when(jnp.logical_not(has_bot))
        def _():
            bot_o[...] = jnp.zeros_like(bot_o)

    with scope("meta"):
        fetches[0].wait()
        own_row = owner[...]
        match = (own_row == iota((n, obs_rows), 0)).astype(F32)
        block = 256 if obs_rows % 256 == 0 else 128
        upper = (iota((block, block), 0) < iota((block, block), 1)).astype(F32).astype(BF16)
        carry = jnp.zeros((n, 1), F32)
        ranks = []
        for start in range(0, obs_rows, block):
            part = match[:, start:start + block]
            before = dot(part.astype(BF16), upper) + carry
            ranks.append(jnp.sum(before * part, axis=0, keepdims=True))
            carry = carry + jnp.sum(part, axis=1, keepdims=True)
        rank = jnp.concatenate(ranks, axis=1).astype(jnp.int32)
        slot_row[...] = own_row * slots + rank
        fetches[1].wait()
        lane = iota((1, obs_rows), 1)
        cells_row = jnp.concatenate([cell[i:i + 1, :] for i in range(obs_rows // 128)], axis=1)
        code = jnp.where(lane < count[0], cells_row + 1, 0)
        high = (code // 128).astype(F32)
        low = lax.rem(code, 128).astype(F32)
        coded = jnp.concatenate([match * high, match * low], axis=0).astype(BF16)
        by_rank = (rank == iota((128, obs_rows), 0)).astype(F32).astype(BF16)
        parts = dot(coded, by_rank, ((1,), (1,)))
        meta[...] = (128.0 * parts[0:n] + parts[n:2 * n]).astype(jnp.int32).reshape(n, 1, 128)
        fetches[2].wait()

    def prepare(first, where):
        base = 0 if where is near else peers
        ids = slot_row[...]
        picks = []
        targets = []
        for u in range(batch):
            _, target = where(first + u)
            targets.append(target)
            rel = jnp.clip(ids - target * slots, -1, slots).astype(F32)
            rel = jnp.broadcast_to(rel, (16, obs_rows)).astype(BF16)
            for at in range(0, slots, 16):
                line = (iota((16, obs_rows), 0) + at).astype(F32).astype(BF16)
                picks.append(jnp.where(rel == line, jnp.ones_like(line), jnp.zeros_like(line)))
        rows = dot(jnp.concatenate(picks, axis=0), obs[...]).astype(BF16)
        for u in range(batch):
            sbuf[base + first + u] = rows[u * slots:(u + 1) * slots]

    def ship_unit(off, where, base):
        to, target = where(off)
        at = base + off
        remote(meta.at[target], meta_r.at[at], meta_send, meta_recv.at[at // batch], to).start()
        remote(sbuf.at[at], rbuf.at[at], row_send, row_recv.at[at // batch], to).start()

    rounds = peers // batch

    def loops(order, body):
        at = 0
        while at < len(order):
            kind, first = order[at]
            last = at + 1
            while last < len(order) and order[last] == (kind, first + last - at):
                last += 1
            if last - at == 1:
                body(kind, first)
            else:
                def step(p, carry, kind=kind):
                    body(kind, p)
                    return carry

                lax.fori_loop(first, first + last - at, step, 0)
            at = last

    def order_of(quarters):
        part = rounds // 4
        return [(kind, q * part + i) for kind, q in quarters for i in range(part)]

    send_order = order_of(SEND)

    def prepare_step(kind, p):
        prepare(p * batch, near if kind == "n" else far)

    def ship_step(kind, p):
        where, base = (near, 0) if kind == "n" else (far, peers)
        own = p == 0 if kind == "n" else jnp.logical_and(p == 0, dense)
        if isinstance(p, int) and p > 0:
            ship_unit(p * batch, where, base)
        else:
            @pl.when(own)
            def _():
                _, target = where(0)
                pltpu.make_async_copy(meta.at[target], meta_r.at[base], meta_recv.at[base // batch]).start()
                pltpu.make_async_copy(sbuf.at[base], rbuf.at[base], row_recv.at[base // batch]).start()

            @pl.when(jnp.logical_not(own))
            def _():
                ship_unit(p * batch, where, base)

        for u in range(1, batch):
            ship_unit(p * batch + u, where, base)

    def both_step(kind, p):
        prepare_step(kind, p)
        ship_step(kind, p)

    ready = rounds // 4 * EARLY
    with scope("prep0"):
        loops(send_order[:ready], prepare_step)

    with scope("cotprep"):
        fetches[3].wait()
        rim = iota((EDGE, channels), 0)
        rows_f = [cot[y].astype(F32) for y in range(own_rows)]
        for j in range(n_lon):
            start, stop = j * tile_cols, (j + 1) * tile_cols
            after, ahead = stop % cols, (start - EDGE) % cols
            mixed = jnp.zeros((EDGE, channels), F32)
            for y in range(own_rows):
                row = rows_f[y]
                ends = jnp.where(
                    rim == 0, row[after:after + EDGE],
                    jnp.where(rim == EDGE - 1, row[ahead:ahead + EDGE], 0.0),
                )
                cot_s[j, y * tile_cols:(y + 1) * tile_cols, :] = cot[y, start:stop, :]
                mixed = mixed + (pltpu.roll(ends, EDGE - 2 * y, 0) if y else ends)
                if y == 0:
                    cot_e[0, j, 0:tile_cols, :] = cot[y, start:stop, :]
                    cot_e[0, j, tile_cols:wide, :] = ends.astype(BF16)
                if y == own_rows - 1:
                    cot_e[1, j, 0:tile_cols, :] = cot[y, start:stop, :]
                    cot_e[1, j, tile_cols:wide, :] = ends.astype(BF16)
            cot_s[j, own_rows * tile_cols:own_rows * tile_cols + EDGE, :] = mixed.astype(BF16)

    with scope("barw"):
        pl.semaphore_wait(barrier, n - 1)

    with scope("ship"):
        def send_edges(far_side):
            def go(e, to_tile, dst, sem):
                to_lat = lax.rem(to_tile + deep, n_lat) if far_side else to_tile
                for j in range(0, n_lon, 1 + far_side):
                    remote(cot_e.at[e, j], dst.at[far_side], edge_send, sem.at[far_side], (to_lat, j)).start()

            @pl.when(jnp.logical_and(lon == n_lon - 1, lat < n_lat - 1))
            def _():
                go(1, lat + 1, cot_top, top_recv)

            @pl.when(jnp.logical_and(lon == 0, lat > 0))
            def _():
                go(0, lat - 1, cot_bot, bot_recv)

        for step in range(1, n_lon):
            remote(cot_s.at[hop(step)], cot_r.at[lon], cot_send, cot_recv.at[0], (lat, hop(step))).start()
        cot_r[lon] = cot_s[lon]
        send_edges(0)
        for step in range(n_lon // 2):
            other = 2 * wrap(lon // 2 + step, n_lon // 2)
            remote(
                cot_s.at[other], cot_r.at[n_lon + lon], cot_send, cot_recv.at[1], (far_lat, other)
            ).start()
        send_edges(1)

        loops(send_order[:ready], ship_step)
    with scope("prep2"):
        loops(send_order[ready:], both_step)

    with scope("clear"):
        for s in range(2):
            for b in range(3):
                for i in (0, 1, tile_rows + 2, tile_rows + 3):
                    moved[s, b, i] = jnp.zeros((wide, channels), F32)
        dep[...] = jnp.zeros_like(dep)
        total[...] = jnp.zeros_like(total)
        bias[...] = jnp.zeros_like(bias)
        gka[...] = jnp.zeros_like(gka)

    def cot_wait(s):
        if s == 0:
            drain(cot_r.at[pl.ds(0, n_lon - 1)], cot_recv.at[0])
        else:
            drain(cot_r.at[pl.ds(0, n_lon)], cot_recv.at[1])

        @pl.when(tile_lat[s] > 0)
        def _():
            drain(cot_top.at[s], top_recv.at[s])

        @pl.when(tile_lat[s] < n_lat - 1)
        def _():
            drain(cot_bot.at[s], bot_recv.at[s])

    half = channels // 2
    for fetch in fetches[4:]:
        fetch.wait()
    tap = taps[...]

    def adjoint(h):
        c32[h, 0] = cot_top[h].astype(F32)
        c32[h, tile_rows + 1] = cot_bot[h].astype(F32)

        def widen(j, carry):
            at = h * n_lon + j
            ends = cot_r[at, own_rows * tile_cols:own_rows * tile_cols + EDGE, :].astype(F32)
            for r in range(own_rows):
                m = j * own_rows + r + 1
                c32[h, m, 0:tile_cols, :] = cot_r[at, r * tile_cols:(r + 1) * tile_cols, :].astype(F32)
                c32[h, m, tile_cols:wide, :] = pltpu.roll(ends, 2 * r, 0) if r else ends
            return carry

        lax.fori_loop(0, n_lon, widen, 0)

        def adjoin(m, carry):
            for c in range(0, channels, half):
                acc = jnp.zeros((tile_cols, half), F32)
                for a in (-1, 0, 1):
                    row = c32[h, m + 1 - a, :, c:c + half]
                    for b in (-1, 0, 1):
                        k = 3 * (a + 1) + b + 1
                        turned = pltpu.roll(row, b % wide, 0) if b else row
                        acc = acc + tap[k:k + 1, c:c + half] * turned[0:tile_cols]
                adj_f[pl.ds(pl.multiple_of(m * tile_cols, 8), tile_cols), c:c + half] = scale * acc
            return carry

        lax.fori_loop(0, tile_rows, adjoin, 0)
        adj_b[h] = adj_f[...].astype(BF16)

    def take(step, count):
        first, size = step * batch, count * batch
        s = first // peers
        with scope("rowwait"):
            for i in range(count):
                drain(meta_r.at[pl.ds(first + i * batch, batch)], meta_recv.at[step + i])
                drain(rbuf.at[pl.ds(first + i * batch, batch)], row_recv.at[step + i])
        rows = jnp.concatenate([rbuf[first + q] for q in range(size)], axis=0)
        codes = jnp.concatenate([meta_r[first + q][:, 0:slots] for q in range(size)], axis=1)
        pick = (codes == iota((cells, size * slots), 0) + 1).astype(F32).astype(BF16)
        upstream = dot(pick, adj_b[s], ((0,), (0,))).astype(BF16)
        x = dot(rows, w_in[...]) + b_in[...]
        square = x * x
        t_val = jnp.tanh(x * (CURVE + (CURVE * BEND) * square))
        upper_half = 0.5 + 0.5 * t_val
        lower_half = 0.5 - 0.5 * t_val
        active = x * upper_half
        hidden = active.astype(BF16)
        slope = upper_half + (active * lower_half) * (2.0 * CURVE + (6.0 * CURVE * BEND) * square)
        encoded = dot(hidden, w_out[...]).astype(BF16)
        dep[s] += dot(pick, encoded)
        back = dot(upstream, w_out[...], ((1,), (1,)))
        pre = (back * slope).astype(BF16)
        total[0:hidden_size, :] += dot(hidden, upstream, ((0,), (0,)))
        total[hidden_size:hidden_size + feat, :] += dot(rows, pre, ((0,), (0,)))
        bias[...] += jnp.sum(pre.astype(F32), axis=0, keepdims=True)

    with scope("cotwaitA"):
        cot_wait(0)
    with scope("adjointA"):
        adjoint(0)

    part = rounds // 4

    def take_pair(g, carry):
        take(2 * part * g, 2 * part)
        return carry

    def take_one(g, carry):
        take(part * g, part)
        return carry

    with scope("take1"):
        lax.fori_loop(0, 1, take_pair, 0)
    with scope("adjointB"):
        @pl.when(dense)
        def _():
            with scope("cotwaitB"):
                cot_wait(1)
            adjoint(1)

        @pl.when(jnp.logical_not(dense))
        def _():
            adj_b[1] = adj_b[0]

    with scope("take2"):
        lax.fori_loop(1, 4 - LATE // 2, take_pair, 0)
    with scope("take3"):
        if LATE:
            lax.fori_loop(8 - LATE, 8, take_one, 0)

    with scope("rssend"):
        for p in range(n_lon):
            tot_b[p] = total[p * piece:(p + 1) * piece, :].astype(BF16)
        for step in range(1, n_lon):
            remote(tot_b.at[hop(step)], rs_r.at[lon], rs_send, rs_recv, (lat, hop(step))).start()

    def spread(h):
        def turn_row(m, carry):
            row = dep[h, pl.ds(pl.multiple_of(m * tile_cols, 8), tile_cols), :]
            row = jnp.concatenate([row, jnp.zeros((EDGE, channels), F32)], axis=0)
            moved[h, 0, m + 2] = pltpu.roll(row, 1, 0)
            moved[h, 1, m + 2] = row
            moved[h, 2, m + 2] = pltpu.roll(row, wide - 1, 0)
            return carry

        lax.fori_loop(0, tile_rows, turn_row, 0)

        def out_row(i, c):
            acc = jnp.zeros((wide, half), F32)
            seen = c32[h, i, :, c:c + half]
            for a in (-1, 0, 1):
                for b in (-1, 0, 1):
                    k = 3 * (a + 1) + b + 1
                    value = moved[h, b + 1, i + 1 + a, :, c:c + half]
                    acc = acc + tap[k:k + 1, c:c + half] * value
                    prod = seen * value
                    folded = prod[0:8]
                    for at in range(8, wide, 8):
                        folded = folded + prod[at:at + 8]
                    gka[k, :, c:c + half] += folded
            return acc

        def strip(j, carry):
            for c in range(0, channels, half):
                mixed = jnp.zeros((EDGE, half), F32)
                for r in range(own_rows):
                    acc = out_row(j * own_rows + r + 1, c)
                    con_s[h, j, r * tile_cols:(r + 1) * tile_cols, c:c + half] = acc[0:tile_cols].astype(BF16)
                    ends = acc[tile_cols:wide]
                    mixed = mixed + (pltpu.roll(ends, EDGE - 2 * r, 0) if r else ends)
                con_s[h, j, own_rows * tile_cols:own_rows * tile_cols + EDGE, c:c + half] = mixed.astype(BF16)
            return carry

        for e, i in ((0, 0), (1, tile_rows + 1)):
            for c in range(0, channels, half):
                con_e[h, e, :, c:c + half] = out_row(i, c).astype(BF16)
        lax.fori_loop(0, n_lon, strip, 0)

    def send_strip(h, step):
        where = lon if h == 0 else n_lon + lon // 2
        remote(
            con_s.at[h, hop(step)], main_o.at[where], con_send, con_recv, (tile_lat[h], hop(step))
        ).start()

    def rim_copy(h, e):
        where = lon if h == 0 else n_lon + lon // 2
        if e == 0:
            return remote(con_e.at[h, 0], bot_o.at[where], rim_send, rim_recv.at[0], (tile_lat[h] - 1, n_lon - 1))
        return remote(con_e.at[h, 1], top_o.at[where], rim_send, rim_recv.at[1], (tile_lat[h] + 1, 0))

    def rims(h, act):
        @pl.when(tile_lat[h] > 0)
        def _():
            act(rim_copy(h, 0))

        @pl.when(tile_lat[h] < n_lat - 1)
        def _():
            act(rim_copy(h, 1))

    first_part = n_lon // 2
    with scope("spread"):
        @pl.when(dense)
        def _():
            spread(1)
            rims(1, lambda copy: copy.start())
            for step in range(first_part):
                send_strip(1, step)

        @pl.when(jnp.logical_not(dense))
        def _():
            dep[0] += dep[1]

        spread(0)
        rims(0, lambda copy: copy.start())

    with scope("misc"):
        grads = [jnp.sum(gka[k], axis=0, keepdims=True) * scale for k in range(len(OFFSETS))]
        spare = misc_s.shape[0] - len(OFFSETS) - 1
        misc_s[...] = jnp.concatenate(
            [bias[...]] + grads + [jnp.zeros((spare, channels), F32)], axis=0
        ).astype(BF16)
        for step in range(1, n_lon):
            remote(misc_s, misc_r.at[lon], mp_send, mp_recv, (lat, hop(step))).start()
        misc_r[lon] = misc_s[...]

    with scope("rswait"):
        drain(rs_r.at[pl.ds(0, n_lon - 1)], rs_recv)
    with scope("zsend"):
        rs_r[lon] = tot_b[lon]
        part = rs_r[0].astype(F32)
        for p in range(1, n_lon):
            part = part + rs_r[p].astype(F32)
        z_s[...] = part.astype(BF16)
        for step in range(1, n_lat):
            remote(z_s, z_r.at[lat], z_send, z_recv, (wrap(lat + step, n_lat), lon)).start()
        z_r[lat] = z_s[...]

        @pl.when(dense)
        def _():
            for step in range(first_part, n_lon):
                send_strip(1, step)

        for step in range(1, n_lon):
            send_strip(0, step)
        main_o[lon] = con_s[0, lon]

    with scope("miscz"):
        drain(misc_r.at[pl.ds(0, n_lon - 1)], mp_recv)
        part = misc_r[0].astype(F32)
        for p in range(1, n_lon):
            part = part + misc_r[p].astype(F32)
        misc_z[...] = part.astype(BF16)
        for step in range(1, n_lat):
            remote(misc_z, misc_o.at[lat], mz_send, mz_recv, (wrap(lat + step, n_lat), lon)).start()
        misc_o[lat] = misc_z[...]

    with scope("zwait"):
        drain(z_r.at[pl.ds(0, n_lat - 1)], z_recv)
    with scope("agsend"):
        part = z_r[0].astype(F32)
        for p in range(1, n_lat):
            part = part + z_r[p].astype(F32)
        fin_s[...] = part.astype(BF16)
        for step in range(1, n_lon):
            remote(fin_s, sums_o.at[lon], ag_send, ag_recv, (lat, hop(step))).start()
        sums_o[lon] = fin_s[...]

    with scope("mzwait"):
        drain(misc_o.at[pl.ds(0, n_lat - 1)], mz_recv)
    with scope("conwait"):
        drain(main_o.at[pl.ds(0, holders - 1)], con_recv)

        @pl.when(has_top)
        def _():
            drain(top_o, rim_recv.at[1])

        @pl.when(has_bot)
        def _():
            drain(bot_o, rim_recv.at[0])
    with scope("grid"):
        value = misc_o[0].astype(F32)
        for z in range(1, n_lat):
            value = value + misc_o[z].astype(F32)
        gb_o[...] = value[0:1]
        gk_o[...] = value[1:1 + len(OFFSETS)]
        here = iota((tile_cols, channels), 0)

        def both(ref, j):
            value = ref[j].astype(F32)
            return value if j % 2 else value + ref[n_lon + j // 2].astype(F32)

        bodies = []
        for j in range(n_lon):
            value = both(main_o, j)
            ends = value[own_rows * tile_cols:own_rows * tile_cols + EDGE]
            rows = []
            for y in range(own_rows):
                body = value[y * tile_cols:(y + 1) * tile_cols]
                right = ends[(EDGE - 2 * y) % EDGE:(EDGE - 2 * y) % EDGE + 1]
                left = ends[EDGE - 1 - 2 * y:EDGE - 2 * y]
                for y_at, source in ((0, top_o), (own_rows - 1, bot_o)):
                    if y == y_at:
                        extra = both(source, j)
                        body = body + extra[0:tile_cols]
                        right = right + extra[tile_cols:tile_cols + 1]
                        left = left + extra[tile_cols + EDGE - 1:tile_cols + EDGE]
                rows.append((body, right, left))
            bodies.append(rows)
        for j in range(n_lon):
            for y in range(own_rows):
                value = bodies[j][y][0]
                value = value + jnp.where(here == 0, bodies[(j - 1) % n_lon][y][1], 0.0)
                value = value + jnp.where(here == tile_cols - 1, bodies[(j + 1) % n_lon][y][2], 0.0)
                grid_o[y, j * tile_cols:(j + 1) * tile_cols, :] = value.astype(BF16)
    with scope("agwait"):
        drain(sums_o.at[pl.ds(0, n_lon - 1)], ag_recv)
    with scope("sums"):
        for p in range(n_lon):
            value = sums_o[p].astype(F32)
            start = p * piece
            for ref, low, high in ((gout_o, 0, hidden_size), (gin_o, hidden_size, n_lon * piece)):
                begin, end = max(start, low), min(start + piece, high)
                if begin < end:
                    ref[begin - low:end - low, :] = value[begin - start:end - start]

    with scope("final"):
        drain(sbuf.at[pl.ds(0, 2 * peers - 2)], row_send)
        drain(meta_r.at[pl.ds(0, 2 * peers - 2)], meta_send)

        @pl.when(jnp.logical_not(dense))
        def _():
            drain(sbuf.at[0], row_send)
            drain(meta_r.at[0], meta_send)

        drain(cot_r.at[pl.ds(0, holders - 1)], cot_send)

        @pl.when(jnp.logical_and(lon == n_lon - 1, lat < n_lat - 1))
        def _():
            drain(top_o, edge_send)

        @pl.when(jnp.logical_and(lon == 0, lat > 0))
        def _():
            drain(top_o, edge_send)

        drain(main_o.at[pl.ds(0, n_lon - 1)], con_send)
        rims(0, lambda copy: copy.wait_send())

        @pl.when(dense)
        def _():
            drain(main_o.at[pl.ds(0, n_lon)], con_send)
            rims(1, lambda copy: copy.wait_send())

        drain(rs_r.at[pl.ds(0, n_lon - 1)], rs_send)
        drain(misc_r.at[pl.ds(0, n_lon - 1)], mp_send)
        drain(z_r.at[pl.ds(0, n_lat - 1)], z_send)
        drain(misc_o.at[pl.ds(0, n_lat - 1)], mz_send)
        drain(sums_o.at[pl.ds(0, n_lon - 1)], ag_send)


def finish(*refs):
    sem, half = refs[-1], (len(refs) - 1) // 2
    copies = [pltpu.make_async_copy(refs[i], refs[half + i], sem.at[i]) for i in range(half)]
    for copy in copies:
        copy.start()
    for copy in copies:
        copy.wait()


def local(
    observations, owner_device, local_cell, valid_counts,
    weight_in, bias_in, weight_out, kernel_taps, cotangent,
):
    n_lat, n_lon = lax.axis_size("lat"), lax.axis_size("lon")
    n = n_lat * n_lon
    obs_rows, feat = observations.shape
    hidden_size, channels = weight_out.shape
    own_rows, cols, _ = cotangent.shape
    tile_rows, tile_cols = own_rows * n_lon, cols // n_lon
    cells = tile_rows * tile_cols
    slots = round_up(2 * obs_rows // n, 16)
    batch = 4 if slots > 48 else 8
    piece = (hidden_size + feat) // n_lon
    taps = kernel_taps.shape[0]
    misc_rows = round_up(taps + 1, 16)
    peers = n // 2
    holders = n_lon + n_lon // 2
    strip_rows = own_rows * tile_cols + EDGE
    wide = tile_cols + EDGE
    scale = 1.0 / math.sqrt(obs_rows * n)
    results = (
        (cotangent.shape, BF16), ((feat, hidden_size), F32), ((1, hidden_size), F32),
        ((hidden_size, channels), F32), ((taps, channels), F32),
    )
    far = functools.partial(pltpu.with_memory_space_constraint, memory_space=pltpu.HBM)
    hbm = pl.BlockSpec(memory_space=pltpu.HBM)
    vmem = pl.BlockSpec(memory_space=pltpu.VMEM)
    dma = pltpu.SemaphoreType.DMA
    V = pltpu.VMEM
    found = pl.pallas_call(
        functools.partial(kernel, n_lat, n_lon, slots, batch, scale),
        out_shape=tuple(V(shape, kind) for shape, kind in results),
        in_specs=[hbm, hbm, hbm, pl.BlockSpec(memory_space=pltpu.SMEM)] + [hbm] * 5,
        out_specs=(vmem,) * 5,
        scratch_shapes=[
            V((obs_rows, feat), BF16), V((1, obs_rows), jnp.int32), V((obs_rows // 128, 128), jnp.int32),
            V((feat, hidden_size), BF16), V((1, hidden_size), F32), V((hidden_size, channels), BF16),
            V((taps, channels), F32), V((own_rows, cols, channels), BF16),
            V((holders, strip_rows, channels), BF16), V((holders, wide, channels), BF16),
            V((holders, wide, channels), BF16), V((n_lon, piece, channels), BF16),
            V((n_lat, misc_rows, channels), BF16),
            V((n, 1, 128), jnp.int32), V((n, 1, 128), jnp.int32), V((1, obs_rows), jnp.int32),
            V((n, slots, feat), BF16), V((n, slots, feat), BF16),
            V((n_lon, strip_rows, channels), BF16), V((2, n_lon, wide, channels), BF16),
            V((2 * n_lon, strip_rows, channels), BF16), V((2, wide, channels), BF16), V((2, wide, channels), BF16),
            V((2, tile_rows + 2, wide, channels), F32), V((cells, channels), F32), V((2, cells, channels), BF16),
            V((2, cells, channels), F32), V((2, 3, tile_rows + 4, wide, channels), F32),
            V((2, n_lon, strip_rows, channels), BF16), V((2, 2, wide, channels), BF16),
            V((taps, 8, channels), F32), V((hidden_size + feat, channels), F32), V((1, hidden_size), F32),
            V((n_lon, piece, channels), BF16), V((n_lon, piece, channels), BF16),
            V((piece, channels), BF16), V((n_lat, piece, channels), BF16), V((piece, channels), BF16),
            V((misc_rows, channels), BF16), V((n_lon, misc_rows, channels), BF16), V((misc_rows, channels), BF16),
            dma((8,)), dma, dma((n // batch,)), dma, dma((n // batch,)), dma, dma((2,)), dma, dma((2,)), dma((2,)),
            dma, dma, dma, dma((2,)), dma, dma, dma, dma, dma, dma,
            dma, dma, dma, dma,
        ],
        compiler_params=pltpu.CompilerParams(
            collective_id=0, has_side_effects=True, vmem_limit_bytes=48 * 1024 * 1024
        ),
    )(
        far(observations), far(owner_device.reshape(1, obs_rows)), far(local_cell.reshape(obs_rows // 128, 128)),
        valid_counts, far(weight_in), far(bias_in.reshape(1, hidden_size)), far(weight_out), far(kernel_taps),
        far(cotangent),
    )
    grid_out, grad_in, grad_bias, grad_out, grad_kernel = pl.pallas_call(
        finish,
        out_shape=tuple(jax.ShapeDtypeStruct(shape, kind) for shape, kind in results),
        in_specs=[vmem] * 5,
        out_specs=(hbm,) * 5,
        scratch_shapes=[dma((5,))],
    )(*[pltpu.with_memory_space_constraint(value, pltpu.VMEM) for value in found])
    return (grid_out, grad_in, grad_bias.reshape(hidden_size), grad_out, grad_kernel)


def solution(mesh):
    return jax.shard_map(
        local,
        mesh=mesh,
        in_specs=(
            P(("lat", "lon"), None),
            P(("lat", "lon"), None),
            P(("lat", "lon")),
            P(("lat", "lon")),
            P(),
            P(),
            P(),
            P(),
            P(("lat", "lon"), None, None),
        ),
        out_specs=(P(("lat", "lon"), None, None), P(), P(), P(), P()),
        check_vma=False,
    )
```

```python
import functools
import math

import jax
import jax.numpy as jnp
from jax import lax
from jax.experimental import pallas as pl
from jax.experimental.pallas import tpu as pltpu
from jax.sharding import PartitionSpec as P

MESH = pl.DeviceIdType.MESH
F32 = jnp.float32
BF16 = jnp.bfloat16
OFFSETS = [(a, b) for a in (-1, 0, 1) for b in (-1, 0, 1)]
CURVE = math.sqrt(2.0 / math.pi)
BEND = 0.044715
EDGE = 8
EARLY = 1
SEND = (("n", 0), ("n", 1), ("n", 2), ("n", 3), ("f", 0), ("f", 1), ("f", 2), ("f", 3))
LATE = 2


def round_up(value, step):
    return -(-value // step) * step


def iota(shape, dim):
    return lax.broadcasted_iota(jnp.int32, shape, dim)


def dot(left, right, contract=((1,), (0,))):
    return lax.dot_general(left, right, (contract, ((), ())), preferred_element_type=F32)


def kernel(
    n_lat, n_lon, slots, batch, scale,
    obs_h, owner_h, cell_h, count, w_in_h, b_in_h, w_out_h, taps_h, cot_h,
    grid_o, gin_o, gb_o, gout_o, gk_o,
    obs, owner, cell, w_in, b_in, w_out, taps, cot,
    main_o, top_o, bot_o, sums_o, misc_o,
    meta, meta_r, slot_row, sbuf, rbuf, cot_s, cot_e, cot_r, cot_top, cot_bot, c32, adj_f, adj_b,
    dep, moved, con_s, con_e, gka, total, bias, tot_b, rs_r, z_s, z_r, fin_s, misc_s, misc_r, misc_z,
    in_sem, sent, meta_recv, row_recv, near_recv, far_recv, top_recv, bot_recv, con_recv, rim_recv, rs_recv, z_recv, ag_recv, mp_recv, mz_recv,
):
    n = n_lat * n_lon
    lat, lon = lax.axis_index("lat"), lax.axis_index("lon")
    me = lat * n_lon + lon
    deep = n_lat // 2
    peers = deep * n_lon
    group, level = lat // deep, lax.rem(lat, deep)
    dense = lax.rem(lon, 2) == 0
    far_lat = lax.rem(lat + deep, n_lat)
    tile_lat = (lat, far_lat)
    obs_rows, feat = obs.shape
    own_rows, cols, channels = cot.shape
    tile_rows, tile_cols = own_rows * n_lon, cols // n_lon
    cells = tile_rows * tile_cols
    wide = tile_cols + EDGE
    hidden_size = w_in.shape[1]
    piece = tot_b.shape[1]
    holders = n_lon + n_lon // 2
    scope = jax.named_scope

    def wrap(value, size):
        return jnp.where(value >= size, value - size, value)

    def hop(step):
        return wrap(lon + step, n_lon)

    def seat(off):
        return wrap(level + off // n_lon, deep), wrap(lon + lax.rem(off, n_lon), n_lon)

    def near(off):
        to_level, to_lon = seat(off)
        to_lat = group * deep + to_level
        return (to_lat, to_lon), to_lat * n_lon + to_lon

    def far(off):
        to_level, to_lon = seat(off)
        to_lat = (1 - group) * deep + to_level
        stand_in = lax.rem(to_lon, 2) == 0
        return (jnp.where(stand_in, group * deep + to_level, to_lat), to_lon), to_lat * n_lon + to_lon

    def remote(src, dst, send, recv, device):
        return pltpu.make_async_remote_copy(
            src_ref=src, dst_ref=dst, send_sem=send, recv_sem=recv,
            device_id=device, device_id_type=MESH,
        )

    def drain(ref, sem):
        pltpu.make_async_copy(ref, ref, sem).wait()

    pairs = [
        (owner_h, owner), (cell_h, cell), (obs_h, obs), (cot_h, cot),
        (w_in_h, w_in), (b_in_h, b_in), (w_out_h, w_out), (taps_h, taps),
    ]
    fetches = [pltpu.make_async_copy(src, dst, in_sem.at[min(i, 4)]) for i, (src, dst) in enumerate(pairs)]
    for fetch in fetches:
        fetch.start()

    barrier = pltpu.get_barrier_semaphore()

    def signal(to_lat, to_lon):
        pl.semaphore_signal(barrier, inc=1, device_id=(to_lat, to_lon), device_id_type=MESH)

    def greet(turn, carry):
        to_lat = wrap(lat + turn, n_lat)
        for step in range(n_lon):
            signal(to_lat, hop(step))
        return carry

    with scope("greet"):
        lax.fori_loop(1, n_lat, greet, 0)
        for step in range(1, n_lon):
            signal(lat, hop(step))

    with scope("zero"):
        for s in range(2):
            @pl.when(tile_lat[s] == 0)
            def _(s=s):
                cot_top[s] = jnp.zeros((wide, channels), BF16)

            @pl.when(tile_lat[s] == n_lat - 1)
            def _(s=s):
                cot_bot[s] = jnp.zeros((wide, channels), BF16)

        has_top = jnp.logical_and(lon == 0, lat > 0)
        has_bot = jnp.logical_and(lon == n_lon - 1, lat < n_lat - 1)

        @pl.when(jnp.logical_not(has_top))
        def _():
            top_o[...] = jnp.zeros_like(top_o)

        @pl.when(jnp.logical_not(has_bot))
        def _():
            bot_o[...] = jnp.zeros_like(bot_o)

    with scope("meta"):
        fetches[0].wait()
        own_row = owner[...]
        match = (own_row == iota((n, obs_rows), 0)).astype(F32)
        block = 256 if obs_rows % 256 == 0 else 128
        upper = (iota((block, block), 0) < iota((block, block), 1)).astype(F32).astype(BF16)
        carry = jnp.zeros((n, 1), F32)
        ranks = []
        for start in range(0, obs_rows, block):
            part = match[:, start:start + block]
            before = dot(part.astype(BF16), upper) + carry
            ranks.append(jnp.sum(before * part, axis=0, keepdims=True))
            carry = carry + jnp.sum(part, axis=1, keepdims=True)
        rank = jnp.concatenate(ranks, axis=1).astype(jnp.int32)
        slot_row[...] = own_row * slots + rank
        fetches[1].wait()
        lane = iota((1, obs_rows), 1)
        cells_row = jnp.concatenate([cell[i:i + 1, :] for i in range(obs_rows // 128)], axis=1)
        code = jnp.where(lane < count[0], cells_row + 1, 0)
        high = (code // 128).astype(F32)
        low = lax.rem(code, 128).astype(F32)
        coded = jnp.concatenate([match * high, match * low], axis=0).astype(BF16)
        by_rank = (rank == iota((128, obs_rows), 0)).astype(F32).astype(BF16)
        parts = dot(coded, by_rank, ((1,), (1,)))
        meta[...] = (128.0 * parts[0:n] + parts[n:2 * n]).astype(jnp.int32).reshape(n, 1, 128)
        fetches[2].wait()

    def prepare(first, where):
        base = 0 if where is near else peers
        ids = slot_row[...]
        picks = []
        targets = []
        for u in range(batch):
            _, target = where(first + u)
            targets.append(target)
            rel = jnp.clip(ids - target * slots, -1, slots).astype(F32)
            rel = jnp.broadcast_to(rel, (16, obs_rows)).astype(BF16)
            for at in range(0, slots, 16):
                line = (iota((16, obs_rows), 0) + at).astype(F32).astype(BF16)
                picks.append(jnp.where(rel == line, jnp.ones_like(line), jnp.zeros_like(line)))
        rows = dot(jnp.concatenate(picks, axis=0), obs[...]).astype(BF16)
        for u in range(batch):
            sbuf[base + first + u] = rows[u * slots:(u + 1) * slots]

    def slot(step):
        quarter = step // (rounds // 4)
        return jnp.where(quarter < 8 - LATE, quarter // 2, quarter - (8 - LATE) // 2)

    def ship_unit(off, where, base):
        to, target = where(off)
        at = base + off
        remote(meta.at[target], meta_r.at[at], sent, meta_recv.at[slot(at // batch)], to).start()
        remote(sbuf.at[at], rbuf.at[at], sent, row_recv.at[slot(at // batch)], to).start()

    rounds = peers // batch

    def loops(order, body):
        at = 0
        while at < len(order):
            kind, first = order[at]
            last = at + 1
            while last < len(order) and order[last] == (kind, first + last - at):
                last += 1
            if last - at == 1:
                body(kind, first)
            else:
                def step(p, carry, kind=kind):
                    body(kind, p)
                    return carry

                lax.fori_loop(first, first + last - at, step, 0)
            at = last

    def order_of(quarters):
        part = rounds // 4
        return [(kind, q * part + i) for kind, q in quarters for i in range(part)]

    send_order = order_of(SEND)

    def prepare_step(kind, p):
        prepare(p * batch, near if kind == "n" else far)

    def ship_step(kind, p):
        where, base = (near, 0) if kind == "n" else (far, peers)
        own = p == 0 if kind == "n" else jnp.logical_and(p == 0, dense)
        if isinstance(p, int) and p > 0:
            ship_unit(p * batch, where, base)
        else:
            @pl.when(own)
            def _():
                _, target = where(0)
                pltpu.make_async_copy(meta.at[target], meta_r.at[base], meta_recv.at[slot(base // batch)]).start()
                pltpu.make_async_copy(sbuf.at[base], rbuf.at[base], row_recv.at[slot(base // batch)]).start()

            @pl.when(jnp.logical_not(own))
            def _():
                ship_unit(p * batch, where, base)

        for u in range(1, batch):
            ship_unit(p * batch + u, where, base)

    def both_step(kind, p):
        prepare_step(kind, p)
        ship_step(kind, p)

    ready = rounds // 4 * EARLY
    with scope("prep0"):
        loops(send_order[:ready], prepare_step)

    with scope("cotprep"):
        fetches[3].wait()
        rim = iota((EDGE, channels), 0)
        rows_f = [cot[y].astype(F32) for y in range(own_rows)]
        for j in range(n_lon):
            start, stop = j * tile_cols, (j + 1) * tile_cols
            after, ahead = stop % cols, (start - EDGE) % cols
            mixed = jnp.zeros((EDGE, channels), F32)
            for y in range(own_rows):
                row = rows_f[y]
                ends = jnp.where(
                    rim == 0, row[after:after + EDGE],
                    jnp.where(rim == EDGE - 1, row[ahead:ahead + EDGE], 0.0),
                )
                cot_s[j, y * tile_cols:(y + 1) * tile_cols, :] = cot[y, start:stop, :]
                mixed = mixed + (pltpu.roll(ends, EDGE - 2 * y, 0) if y else ends)
                if y == 0:
                    cot_e[0, j, 0:tile_cols, :] = cot[y, start:stop, :]
                    cot_e[0, j, tile_cols:wide, :] = ends.astype(BF16)
                if y == own_rows - 1:
                    cot_e[1, j, 0:tile_cols, :] = cot[y, start:stop, :]
                    cot_e[1, j, tile_cols:wide, :] = ends.astype(BF16)
            cot_s[j, own_rows * tile_cols:own_rows * tile_cols + EDGE, :] = mixed.astype(BF16)

    with scope("barw"):
        pl.semaphore_wait(barrier, n - 1)

    with scope("ship"):
        def send_edges(far_side):
            def go(e, to_tile, dst, sem):
                to_lat = lax.rem(to_tile + deep, n_lat) if far_side else to_tile
                for j in range(0, n_lon, 1 + far_side):
                    remote(cot_e.at[e, j], dst.at[far_side], sent, sem.at[far_side], (to_lat, j)).start()

            @pl.when(jnp.logical_and(lon == n_lon - 1, lat < n_lat - 1))
            def _():
                go(1, lat + 1, cot_top, top_recv)

            @pl.when(jnp.logical_and(lon == 0, lat > 0))
            def _():
                go(0, lat - 1, cot_bot, bot_recv)

        for step in range(1, n_lon):
            remote(cot_s.at[hop(step)], cot_r.at[lon], sent, near_recv, (lat, hop(step))).start()
        cot_r[lon] = cot_s[lon]
        send_edges(0)
        for step in range(n_lon // 2):
            other = 2 * wrap(lon // 2 + step, n_lon // 2)
            remote(
                cot_s.at[other], cot_r.at[n_lon + lon], sent, far_recv, (far_lat, other)
            ).start()
        send_edges(1)

        loops(send_order[:ready], ship_step)
    with scope("prep2"):
        loops(send_order[ready:], both_step)

    with scope("clear"):
        for s in range(2):
            for b in range(3):
                for i in (0, 1, tile_rows + 2, tile_rows + 3):
                    moved[s, b, i] = jnp.zeros((wide, channels), F32)
        dep[...] = jnp.zeros_like(dep)
        total[...] = jnp.zeros_like(total)
        bias[...] = jnp.zeros_like(bias)
        gka[...] = jnp.zeros_like(gka)

    def cot_wait(s):
        if s == 0:
            drain(cot_r.at[pl.ds(0, n_lon - 1)], near_recv)
        else:
            drain(cot_r.at[pl.ds(0, n_lon)], far_recv)

        @pl.when(tile_lat[s] > 0)
        def _():
            drain(cot_top.at[s], top_recv.at[s])

        @pl.when(tile_lat[s] < n_lat - 1)
        def _():
            drain(cot_bot.at[s], bot_recv.at[s])

    half = channels // 2
    for fetch in fetches[4:]:
        fetch.wait()
    tap = taps[...]

    def adjoint(h):
        c32[h, 0] = cot_top[h].astype(F32)
        c32[h, tile_rows + 1] = cot_bot[h].astype(F32)

        def widen(j, carry):
            at = h * n_lon + j
            ends = cot_r[at, own_rows * tile_cols:own_rows * tile_cols + EDGE, :].astype(F32)
            for r in range(own_rows):
                m = j * own_rows + r + 1
                c32[h, m, 0:tile_cols, :] = cot_r[at, r * tile_cols:(r + 1) * tile_cols, :].astype(F32)
                c32[h, m, tile_cols:wide, :] = pltpu.roll(ends, 2 * r, 0) if r else ends
            return carry

        lax.fori_loop(0, n_lon, widen, 0)

        def adjoin(m, carry):
            for c in range(0, channels, half):
                acc = jnp.zeros((tile_cols, half), F32)
                for a in (-1, 0, 1):
                    row = c32[h, m + 1 - a, :, c:c + half]
                    for b in (-1, 0, 1):
                        k = 3 * (a + 1) + b + 1
                        turned = pltpu.roll(row, b % wide, 0) if b else row
                        acc = acc + tap[k:k + 1, c:c + half] * turned[0:tile_cols]
                adj_f[pl.ds(pl.multiple_of(m * tile_cols, 8), tile_cols), c:c + half] = scale * acc
            return carry

        lax.fori_loop(0, tile_rows, adjoin, 0)
        adj_b[h] = adj_f[...].astype(BF16)

    def take(step, count):
        first, size = step * batch, count * batch
        s = first // peers
        with scope("rowwait"):
            drain(meta_r.at[pl.ds(first, size)], meta_recv.at[slot(step)])
            drain(rbuf.at[pl.ds(first, size)], row_recv.at[slot(step)])
        rows = jnp.concatenate([rbuf[first + q] for q in range(size)], axis=0)
        codes = jnp.concatenate([meta_r[first + q][:, 0:slots] for q in range(size)], axis=1)
        pick = (codes == iota((cells, size * slots), 0) + 1).astype(F32).astype(BF16)
        upstream = dot(pick, adj_b[s], ((0,), (0,))).astype(BF16)
        x = dot(rows, w_in[...]) + b_in[...]
        square = x * x
        t_val = jnp.tanh(x * (CURVE + (CURVE * BEND) * square))
        upper_half = 0.5 + 0.5 * t_val
        lower_half = 0.5 - 0.5 * t_val
        active = x * upper_half
        hidden = active.astype(BF16)
        slope = upper_half + (active * lower_half) * (2.0 * CURVE + (6.0 * CURVE * BEND) * square)
        encoded = dot(hidden, w_out[...]).astype(BF16)
        dep[s] += dot(pick, encoded)
        back = dot(upstream, w_out[...], ((1,), (1,)))
        pre = (back * slope).astype(BF16)
        total[0:hidden_size, :] += dot(hidden, upstream, ((0,), (0,)))
        total[hidden_size:hidden_size + feat, :] += dot(rows, pre, ((0,), (0,)))
        bias[...] += jnp.sum(pre.astype(F32), axis=0, keepdims=True)

    with scope("cotwaitA"):
        cot_wait(0)
    with scope("adjointA"):
        adjoint(0)

    part = rounds // 4

    def take_pair(g, carry):
        take(2 * part * g, 2 * part)
        return carry

    def take_one(g, carry):
        take(part * g, part)
        return carry

    with scope("take1"):
        lax.fori_loop(0, 1, take_pair, 0)
    with scope("adjointB"):
        @pl.when(dense)
        def _():
            with scope("cotwaitB"):
                cot_wait(1)
            adjoint(1)

        @pl.when(jnp.logical_not(dense))
        def _():
            adj_b[1] = adj_b[0]

    with scope("take2"):
        lax.fori_loop(1, 4 - LATE // 2, take_pair, 0)
    with scope("take3"):
        if LATE:
            lax.fori_loop(8 - LATE, 8, take_one, 0)

    with scope("rssend"):
        for p in range(n_lon):
            tot_b[p] = total[p * piece:(p + 1) * piece, :].astype(BF16)
        for step in range(1, n_lon):
            remote(tot_b.at[hop(step)], rs_r.at[lon], sent, rs_recv, (lat, hop(step))).start()

    def spread(h):
        def turn_row(m, carry):
            row = dep[h, pl.ds(pl.multiple_of(m * tile_cols, 8), tile_cols), :]
            row = jnp.concatenate([row, jnp.zeros((EDGE, channels), F32)], axis=0)
            moved[h, 0, m + 2] = pltpu.roll(row, 1, 0)
            moved[h, 1, m + 2] = row
            moved[h, 2, m + 2] = pltpu.roll(row, wide - 1, 0)
            return carry

        lax.fori_loop(0, tile_rows, turn_row, 0)

        def out_row(i, c):
            acc = jnp.zeros((wide, half), F32)
            seen = c32[h, i, :, c:c + half]
            for a in (-1, 0, 1):
                for b in (-1, 0, 1):
                    k = 3 * (a + 1) + b + 1
                    value = moved[h, b + 1, i + 1 + a, :, c:c + half]
                    acc = acc + tap[k:k + 1, c:c + half] * value
                    prod = seen * value
                    folded = prod[0:8]
                    for at in range(8, wide, 8):
                        folded = folded + prod[at:at + 8]
                    gka[k, :, c:c + half] += folded
            return acc

        def strip(j, carry):
            for c in range(0, channels, half):
                mixed = jnp.zeros((EDGE, half), F32)
                for r in range(own_rows):
                    acc = out_row(j * own_rows + r + 1, c)
                    con_s[h, j, r * tile_cols:(r + 1) * tile_cols, c:c + half] = acc[0:tile_cols].astype(BF16)
                    ends = acc[tile_cols:wide]
                    mixed = mixed + (pltpu.roll(ends, EDGE - 2 * r, 0) if r else ends)
                con_s[h, j, own_rows * tile_cols:own_rows * tile_cols + EDGE, c:c + half] = mixed.astype(BF16)
            return carry

        for e, i in ((0, 0), (1, tile_rows + 1)):
            for c in range(0, channels, half):
                con_e[h, e, :, c:c + half] = out_row(i, c).astype(BF16)
        lax.fori_loop(0, n_lon, strip, 0)

    def send_strip(h, step):
        where = lon if h == 0 else n_lon + lon // 2
        remote(
            con_s.at[h, hop(step)], main_o.at[where], sent, con_recv, (tile_lat[h], hop(step))
        ).start()

    def rim_copy(h, e):
        where = lon if h == 0 else n_lon + lon // 2
        if e == 0:
            return remote(con_e.at[h, 0], bot_o.at[where], sent, rim_recv, (tile_lat[h] - 1, n_lon - 1))
        return remote(con_e.at[h, 1], top_o.at[where], sent, rim_recv, (tile_lat[h] + 1, 0))

    def rims(h, act):
        @pl.when(tile_lat[h] > 0)
        def _():
            act(rim_copy(h, 0))

        @pl.when(tile_lat[h] < n_lat - 1)
        def _():
            act(rim_copy(h, 1))

    first_part = n_lon // 2
    with scope("spread"):
        @pl.when(dense)
        def _():
            spread(1)
            rims(1, lambda copy: copy.start())
            for step in range(first_part):
                send_strip(1, step)

        @pl.when(jnp.logical_not(dense))
        def _():
            dep[0] += dep[1]

        spread(0)
        rims(0, lambda copy: copy.start())

    with scope("misc"):
        grads = [jnp.sum(gka[k], axis=0, keepdims=True) * scale for k in range(len(OFFSETS))]
        spare = misc_s.shape[0] - len(OFFSETS) - 1
        misc_s[...] = jnp.concatenate(
            [bias[...]] + grads + [jnp.zeros((spare, channels), F32)], axis=0
        ).astype(BF16)
        for step in range(1, n_lon):
            remote(misc_s, misc_r.at[lon], sent, mp_recv, (lat, hop(step))).start()
        misc_r[lon] = misc_s[...]

    with scope("rswait"):
        drain(rs_r.at[pl.ds(0, n_lon - 1)], rs_recv)
    with scope("zsend"):
        rs_r[lon] = tot_b[lon]
        part = rs_r[0].astype(F32)
        for p in range(1, n_lon):
            part = part + rs_r[p].astype(F32)
        z_s[...] = part.astype(BF16)
        for step in range(1, n_lat):
            remote(z_s, z_r.at[lat], sent, z_recv, (wrap(lat + step, n_lat), lon)).start()
        z_r[lat] = z_s[...]

        @pl.when(dense)
        def _():
            for step in range(first_part, n_lon):
                send_strip(1, step)

        for step in range(1, n_lon):
            send_strip(0, step)
        main_o[lon] = con_s[0, lon]

    with scope("miscz"):
        drain(misc_r.at[pl.ds(0, n_lon - 1)], mp_recv)
        part = misc_r[0].astype(F32)
        for p in range(1, n_lon):
            part = part + misc_r[p].astype(F32)
        misc_z[...] = part.astype(BF16)
        for step in range(1, n_lat):
            remote(misc_z, misc_o.at[lat], sent, mz_recv, (wrap(lat + step, n_lat), lon)).start()
        misc_o[lat] = misc_z[...]

    with scope("zwait"):
        drain(z_r.at[pl.ds(0, n_lat - 1)], z_recv)
    with scope("agsend"):
        part = z_r[0].astype(F32)
        for p in range(1, n_lat):
            part = part + z_r[p].astype(F32)
        fin_s[...] = part.astype(BF16)
        for step in range(1, n_lon):
            remote(fin_s, sums_o.at[lon], sent, ag_recv, (lat, hop(step))).start()
        sums_o[lon] = fin_s[...]

    with scope("mzwait"):
        drain(misc_o.at[pl.ds(0, n_lat - 1)], mz_recv)
    with scope("conwait"):
        drain(main_o.at[pl.ds(0, holders - 1)], con_recv)

        @pl.when(has_top)
        def _():
            drain(top_o, rim_recv)

        @pl.when(has_bot)
        def _():
            drain(bot_o, rim_recv)
    with scope("grid"):
        value = misc_o[0].astype(F32)
        for z in range(1, n_lat):
            value = value + misc_o[z].astype(F32)
        gb_o[...] = value[0:1]
        gk_o[...] = value[1:1 + len(OFFSETS)]
        here = iota((tile_cols, channels), 0)

        def both(ref, j):
            value = ref[j].astype(F32)
            return value if j % 2 else value + ref[n_lon + j // 2].astype(F32)

        bodies = []
        for j in range(n_lon):
            value = both(main_o, j)
            ends = value[own_rows * tile_cols:own_rows * tile_cols + EDGE]
            rows = []
            for y in range(own_rows):
                body = value[y * tile_cols:(y + 1) * tile_cols]
                right = ends[(EDGE - 2 * y) % EDGE:(EDGE - 2 * y) % EDGE + 1]
                left = ends[EDGE - 1 - 2 * y:EDGE - 2 * y]
                for y_at, source in ((0, top_o), (own_rows - 1, bot_o)):
                    if y == y_at:
                        extra = both(source, j)
                        body = body + extra[0:tile_cols]
                        right = right + extra[tile_cols:tile_cols + 1]
                        left = left + extra[tile_cols + EDGE - 1:tile_cols + EDGE]
                rows.append((body, right, left))
            bodies.append(rows)
        for j in range(n_lon):
            for y in range(own_rows):
                value = bodies[j][y][0]
                value = value + jnp.where(here == 0, bodies[(j - 1) % n_lon][y][1], 0.0)
                value = value + jnp.where(here == tile_cols - 1, bodies[(j + 1) % n_lon][y][2], 0.0)
                grid_o[y, j * tile_cols:(j + 1) * tile_cols, :] = value.astype(BF16)
    with scope("agwait"):
        drain(sums_o.at[pl.ds(0, n_lon - 1)], ag_recv)
    with scope("sums"):
        for p in range(n_lon):
            value = sums_o[p].astype(F32)
            start = p * piece
            for ref, low, high in ((gout_o, 0, hidden_size), (gin_o, hidden_size, n_lon * piece)):
                begin, end = max(start, low), min(start + piece, high)
                if begin < end:
                    ref[begin - low:end - low, :] = value[begin - start:end - start]

    with scope("final"):
        drain(sbuf.at[pl.ds(0, 2 * peers - 2)], sent)
        drain(meta_r.at[pl.ds(0, 2 * peers - 2)], sent)

        @pl.when(jnp.logical_not(dense))
        def _():
            drain(sbuf.at[0], sent)
            drain(meta_r.at[0], sent)

        drain(cot_r.at[pl.ds(0, holders - 1)], sent)

        @pl.when(jnp.logical_and(lon == n_lon - 1, lat < n_lat - 1))
        def _():
            drain(top_o, sent)

        @pl.when(jnp.logical_and(lon == 0, lat > 0))
        def _():
            drain(top_o, sent)

        drain(main_o.at[pl.ds(0, n_lon - 1)], sent)
        rims(0, lambda copy: copy.wait_send())

        @pl.when(dense)
        def _():
            drain(main_o.at[pl.ds(0, n_lon)], sent)
            rims(1, lambda copy: copy.wait_send())

        drain(rs_r.at[pl.ds(0, n_lon - 1)], sent)
        drain(misc_r.at[pl.ds(0, n_lon - 1)], sent)
        drain(z_r.at[pl.ds(0, n_lat - 1)], sent)
        drain(misc_o.at[pl.ds(0, n_lat - 1)], sent)
        drain(sums_o.at[pl.ds(0, n_lon - 1)], sent)


def finish(*refs):
    sem, half = refs[-1], (len(refs) - 1) // 2
    copies = [pltpu.make_async_copy(refs[i], refs[half + i], sem) for i in range(half)]
    for copy in copies:
        copy.start()
    for copy in copies:
        copy.wait()


def local(
    observations, owner_device, local_cell, valid_counts,
    weight_in, bias_in, weight_out, kernel_taps, cotangent,
):
    n_lat, n_lon = lax.axis_size("lat"), lax.axis_size("lon")
    n = n_lat * n_lon
    obs_rows, feat = observations.shape
    hidden_size, channels = weight_out.shape
    own_rows, cols, _ = cotangent.shape
    tile_rows, tile_cols = own_rows * n_lon, cols // n_lon
    cells = tile_rows * tile_cols
    slots = round_up(2 * obs_rows // n, 16)
    batch = 4 if slots > 48 else 8
    piece = (hidden_size + feat) // n_lon
    taps = kernel_taps.shape[0]
    misc_rows = round_up(taps + 1, 16)
    peers = n // 2
    holders = n_lon + n_lon // 2
    strip_rows = own_rows * tile_cols + EDGE
    wide = tile_cols + EDGE
    scale = 1.0 / math.sqrt(obs_rows * n)
    results = (
        (cotangent.shape, BF16), ((feat, hidden_size), F32), ((1, hidden_size), F32),
        ((hidden_size, channels), F32), ((taps, channels), F32),
    )
    far = functools.partial(pltpu.with_memory_space_constraint, memory_space=pltpu.HBM)
    hbm = pl.BlockSpec(memory_space=pltpu.HBM)
    vmem = pl.BlockSpec(memory_space=pltpu.VMEM)
    dma = pltpu.SemaphoreType.DMA
    V = pltpu.VMEM
    found = pl.pallas_call(
        functools.partial(kernel, n_lat, n_lon, slots, batch, scale),
        out_shape=tuple(V(shape, kind) for shape, kind in results),
        in_specs=[hbm, hbm, hbm, pl.BlockSpec(memory_space=pltpu.SMEM)] + [hbm] * 5,
        out_specs=(vmem,) * 5,
        scratch_shapes=[
            V((obs_rows, feat), BF16), V((1, obs_rows), jnp.int32), V((obs_rows // 128, 128), jnp.int32),
            V((feat, hidden_size), BF16), V((1, hidden_size), F32), V((hidden_size, channels), BF16),
            V((taps, channels), F32), V((own_rows, cols, channels), BF16),
            V((holders, strip_rows, channels), BF16), V((holders, wide, channels), BF16),
            V((holders, wide, channels), BF16), V((n_lon, piece, channels), BF16),
            V((n_lat, misc_rows, channels), BF16),
            V((n, 1, 128), jnp.int32), V((n, 1, 128), jnp.int32), V((1, obs_rows), jnp.int32),
            V((n, slots, feat), BF16), V((n, slots, feat), BF16),
            V((n_lon, strip_rows, channels), BF16), V((2, n_lon, wide, channels), BF16),
            V((2 * n_lon, strip_rows, channels), BF16), V((2, wide, channels), BF16), V((2, wide, channels), BF16),
            V((2, tile_rows + 2, wide, channels), F32), V((cells, channels), F32), V((2, cells, channels), BF16),
            V((2, cells, channels), F32), V((2, 3, tile_rows + 4, wide, channels), F32),
            V((2, n_lon, strip_rows, channels), BF16), V((2, 2, wide, channels), BF16),
            V((taps, 8, channels), F32), V((hidden_size + feat, channels), F32), V((1, hidden_size), F32),
            V((n_lon, piece, channels), BF16), V((n_lon, piece, channels), BF16),
            V((piece, channels), BF16), V((n_lat, piece, channels), BF16), V((piece, channels), BF16),
            V((misc_rows, channels), BF16), V((n_lon, misc_rows, channels), BF16), V((misc_rows, channels), BF16),
            dma((5,)), dma, dma((4 + LATE // 2,)), dma((4 + LATE // 2,)), dma, dma, dma((2,)), dma((2,)),
            dma, dma, dma, dma, dma, dma, dma,
        ],
        compiler_params=pltpu.CompilerParams(
            collective_id=0, has_side_effects=True, vmem_limit_bytes=48 * 1024 * 1024
        ),
    )(
        far(observations), far(owner_device.reshape(1, obs_rows)), far(local_cell.reshape(obs_rows // 128, 128)),
        valid_counts, far(weight_in), far(bias_in.reshape(1, hidden_size)), far(weight_out), far(kernel_taps),
        far(cotangent),
    )
    grid_out, grad_in, grad_bias, grad_out, grad_kernel = pl.pallas_call(
        finish,
        out_shape=tuple(jax.ShapeDtypeStruct(shape, kind) for shape, kind in results),
        in_specs=[vmem] * 5,
        out_specs=(hbm,) * 5,
        scratch_shapes=[dma],
    )(*[pltpu.with_memory_space_constraint(value, pltpu.VMEM) for value in found])
    return (grid_out, grad_in, grad_bias.reshape(hidden_size), grad_out, grad_kernel)


def solution(mesh):
    return jax.shard_map(
        local,
        mesh=mesh,
        in_specs=(
            P(("lat", "lon"), None),
            P(("lat", "lon"), None),
            P(("lat", "lon")),
            P(("lat", "lon")),
            P(),
            P(),
            P(),
            P(),
            P(("lat", "lon"), None, None),
        ),
        out_specs=(P(("lat", "lon"), None, None), P(), P(), P(), P()),
        check_vma=False,
    )
```

```python
import functools
import math

import jax
import jax.numpy as jnp
from jax import lax
from jax.experimental import pallas as pl
from jax.experimental.pallas import tpu as pltpu
from jax.sharding import PartitionSpec as P

MESH = pl.DeviceIdType.MESH
F32 = jnp.float32
BF16 = jnp.bfloat16
OFFSETS = [(a, b) for a in (-1, 0, 1) for b in (-1, 0, 1)]
CURVE = math.sqrt(2.0 / math.pi)
BEND = 0.044715
EDGE = 8
EARLY = 1
SEND = (("n", 0), ("n", 1), ("n", 2), ("n", 3), ("f", 0), ("f", 1), ("f", 2), ("f", 3))
LATE = 2


def round_up(value, step):
    return -(-value // step) * step


def iota(shape, dim):
    return lax.broadcasted_iota(jnp.int32, shape, dim)


def dot(left, right, contract=((1,), (0,))):
    return lax.dot_general(left, right, (contract, ((), ())), preferred_element_type=F32)


def kernel(
    n_lat, n_lon, slots, batch, scale,
    obs_h, owner_h, cell_h, count, w_in_h, b_in_h, w_out_h, taps_h, cot_h,
    grid_o, gin_o, gb_o, gout_o, gk_o,
    obs, owner, cell, w_in, b_in, w_out, taps, cot,
    main_o, top_o, bot_o, sums_o, misc_o,
    meta, meta_r, slot_row, sbuf, rbuf, cot_s, cot_e, cot_r, cot_top, cot_bot, c32, adj_f, adj_b,
    dep, moved, con_s, con_e, gka, total, bias, tot_b, rs_r, z_s, z_r, fin_s, misc_s, misc_r, misc_z,
    in_sem, sent, meta_recv, row_recv, near_recv, far_recv, top_recv, bot_recv, con_recv, rim_recv, rs_recv, z_recv, ag_recv, mp_recv, mz_recv,
):
    n = n_lat * n_lon
    lat, lon = lax.axis_index("lat"), lax.axis_index("lon")
    me = lat * n_lon + lon
    deep = n_lat // 2
    peers = deep * n_lon
    group, level = lat // deep, lax.rem(lat, deep)
    dense = lax.rem(lon, 2) == 0
    far_lat = lax.rem(lat + deep, n_lat)
    tile_lat = (lat, far_lat)
    obs_rows, feat = obs.shape
    own_rows, cols, channels = cot.shape
    tile_rows, tile_cols = own_rows * n_lon, cols // n_lon
    cells = tile_rows * tile_cols
    wide = tile_cols + EDGE
    hidden_size = w_in.shape[1]
    piece = tot_b.shape[1]
    holders = n_lon + n_lon // 2
    scope = jax.named_scope

    def wrap(value, size):
        return jnp.where(value >= size, value - size, value)

    def hop(step):
        return wrap(lon + step, n_lon)

    def seat(off):
        return wrap(level + off // n_lon, deep), wrap(lon + lax.rem(off, n_lon), n_lon)

    def near(off):
        to_level, to_lon = seat(off)
        to_lat = group * deep + to_level
        return (to_lat, to_lon), to_lat * n_lon + to_lon

    def far(off):
        to_level, to_lon = seat(off)
        to_lat = (1 - group) * deep + to_level
        stand_in = lax.rem(to_lon, 2) == 0
        return (jnp.where(stand_in, group * deep + to_level, to_lat), to_lon), to_lat * n_lon + to_lon

    def remote(src, dst, send, recv, device):
        return pltpu.make_async_remote_copy(
            src_ref=src, dst_ref=dst, send_sem=send, recv_sem=recv,
            device_id=device, device_id_type=MESH,
        )

    def drain(ref, sem):
        pltpu.make_async_copy(ref, ref, sem).wait()

    pairs = [
        (owner_h, owner), (cell_h, cell), (obs_h, obs), (cot_h, cot),
        (w_in_h, w_in), (b_in_h, b_in), (w_out_h, w_out), (taps_h, taps),
    ]
    fetches = [pltpu.make_async_copy(src, dst, in_sem.at[min(i, 4)]) for i, (src, dst) in enumerate(pairs)]
    for fetch in fetches:
        fetch.start()

    barrier = pltpu.get_barrier_semaphore()

    def signal(to_lat, to_lon):
        pl.semaphore_signal(barrier, inc=1, device_id=(to_lat, to_lon), device_id_type=MESH)

    def greet(turn, carry):
        to_lat = wrap(lat + turn, n_lat)
        for step in range(n_lon):
            signal(to_lat, hop(step))
        return carry

    with scope("greet"):
        lax.fori_loop(1, n_lat, greet, 0)
        for step in range(1, n_lon):
            signal(lat, hop(step))

    with scope("zero"):
        for s in range(2):
            @pl.when(tile_lat[s] == 0)
            def _(s=s):
                cot_top[s] = jnp.zeros((wide, channels), BF16)

            @pl.when(tile_lat[s] == n_lat - 1)
            def _(s=s):
                cot_bot[s] = jnp.zeros((wide, channels), BF16)

        has_top = jnp.logical_and(lon == 0, lat > 0)
        has_bot = jnp.logical_and(lon == n_lon - 1, lat < n_lat - 1)

        @pl.when(jnp.logical_not(has_top))
        def _():
            top_o[...] = jnp.zeros_like(top_o)

        @pl.when(jnp.logical_not(has_bot))
        def _():
            bot_o[...] = jnp.zeros_like(bot_o)

    with scope("meta"):
        fetches[0].wait()
        own_row = owner[...]
        match = (own_row == iota((n, obs_rows), 0)).astype(F32)
        block = 256 if obs_rows % 256 == 0 else 128
        upper = (iota((block, block), 0) < iota((block, block), 1)).astype(F32).astype(BF16)
        carry = jnp.zeros((n, 1), F32)
        ranks = []
        for start in range(0, obs_rows, block):
            part = match[:, start:start + block]
            before = dot(part.astype(BF16), upper) + carry
            ranks.append(jnp.sum(before * part, axis=0, keepdims=True))
            carry = carry + jnp.sum(part, axis=1, keepdims=True)
        rank = jnp.concatenate(ranks, axis=1).astype(jnp.int32)
        slot_row[...] = own_row * slots + rank
        fetches[1].wait()
        lane = iota((1, obs_rows), 1)
        cells_row = jnp.concatenate([cell[i:i + 1, :] for i in range(obs_rows // 128)], axis=1)
        code = jnp.where(lane < count[0], cells_row + 1, 0)
        high = (code // 128).astype(F32)
        low = lax.rem(code, 128).astype(F32)
        coded = jnp.concatenate([match * high, match * low], axis=0).astype(BF16)
        by_rank = (rank == iota((128, obs_rows), 0)).astype(F32).astype(BF16)
        parts = dot(coded, by_rank, ((1,), (1,)))
        meta[...] = (128.0 * parts[0:n] + parts[n:2 * n]).astype(jnp.int32).reshape(n, 1, 128)
        fetches[2].wait()

    def prepare(first, where):
        base = 0 if where is near else peers
        ids = slot_row[...]
        picks = []
        targets = []
        for u in range(batch):
            _, target = where(first + u)
            targets.append(target)
            rel = jnp.clip(ids - target * slots, -1, slots).astype(F32)
            rel = jnp.broadcast_to(rel, (16, obs_rows)).astype(BF16)
            for at in range(0, slots, 16):
                line = (iota((16, obs_rows), 0) + at).astype(F32).astype(BF16)
                picks.append(jnp.where(rel == line, jnp.ones_like(line), jnp.zeros_like(line)))
        rows = dot(jnp.concatenate(picks, axis=0), obs[...]).astype(BF16)
        for u in range(batch):
            sbuf[base + first + u] = rows[u * slots:(u + 1) * slots]

    def slot(step):
        quarter = step // (rounds // 4)
        return jnp.where(quarter < 8 - LATE, quarter // 2, quarter - (8 - LATE) // 2)

    def ship_unit(off, where, base):
        to, target = where(off)
        at = base + off
        remote(meta.at[target], meta_r.at[at], sent, meta_recv.at[slot(at // batch)], to).start()
        remote(sbuf.at[at], rbuf.at[at], sent, row_recv.at[slot(at // batch)], to).start()

    rounds = peers // batch

    def loops(order, body):
        at = 0
        while at < len(order):
            kind, first = order[at]
            last = at + 1
            while last < len(order) and order[last] == (kind, first + last - at):
                last += 1
            if last - at == 1:
                body(kind, first)
            else:
                def step(p, carry, kind=kind):
                    body(kind, p)
                    return carry

                lax.fori_loop(first, first + last - at, step, 0)
            at = last

    def order_of(quarters):
        part = rounds // 4
        return [(kind, q * part + i) for kind, q in quarters for i in range(part)]

    send_order = order_of(SEND)

    def prepare_step(kind, p):
        prepare(p * batch, near if kind == "n" else far)

    def ship_step(kind, p):
        where, base = (near, 0) if kind == "n" else (far, peers)
        own = p == 0 if kind == "n" else jnp.logical_and(p == 0, dense)
        if isinstance(p, int) and p > 0:
            ship_unit(p * batch, where, base)
        else:
            @pl.when(own)
            def _():
                _, target = where(0)
                pltpu.make_async_copy(meta.at[target], meta_r.at[base], meta_recv.at[slot(base // batch)]).start()
                pltpu.make_async_copy(sbuf.at[base], rbuf.at[base], row_recv.at[slot(base // batch)]).start()

            @pl.when(jnp.logical_not(own))
            def _():
                ship_unit(p * batch, where, base)

        for u in range(1, batch):
            ship_unit(p * batch + u, where, base)

    def both_step(kind, p):
        prepare_step(kind, p)
        ship_step(kind, p)

    ready = rounds // 4 * EARLY
    with scope("prep0"):
        loops(send_order[:ready], prepare_step)

    with scope("cotprep"):
        fetches[3].wait()
        rim = iota((EDGE, channels), 0)
        rows_f = [cot[y].astype(F32) for y in range(own_rows)]
        for j in range(n_lon):
            start, stop = j * tile_cols, (j + 1) * tile_cols
            after, ahead = stop % cols, (start - EDGE) % cols
            mixed = jnp.zeros((EDGE, channels), F32)
            for y in range(own_rows):
                row = rows_f[y]
                ends = jnp.where(
                    rim == 0, row[after:after + EDGE],
                    jnp.where(rim == EDGE - 1, row[ahead:ahead + EDGE], 0.0),
                )
                cot_s[j, y * tile_cols:(y + 1) * tile_cols, :] = cot[y, start:stop, :]
                mixed = mixed + (pltpu.roll(ends, EDGE - 2 * y, 0) if y else ends)
                if y == 0:
                    cot_e[0, j, 0:tile_cols, :] = cot[y, start:stop, :]
                    cot_e[0, j, tile_cols:wide, :] = ends.astype(BF16)
                if y == own_rows - 1:
                    cot_e[1, j, 0:tile_cols, :] = cot[y, start:stop, :]
                    cot_e[1, j, tile_cols:wide, :] = ends.astype(BF16)
            cot_s[j, own_rows * tile_cols:own_rows * tile_cols + EDGE, :] = mixed.astype(BF16)

    with scope("barw"):
        pl.semaphore_wait(barrier, n - 1)

    with scope("ship"):
        def send_edges(far_side):
            def go(e, to_tile, dst, sem):
                to_lat = lax.rem(to_tile + deep, n_lat) if far_side else to_tile
                for j in range(0, n_lon, 1 + far_side):
                    remote(cot_e.at[e, j], dst.at[far_side], sent, sem.at[far_side], (to_lat, j)).start()

            @pl.when(jnp.logical_and(lon == n_lon - 1, lat < n_lat - 1))
            def _():
                go(1, lat + 1, cot_top, top_recv)

            @pl.when(jnp.logical_and(lon == 0, lat > 0))
            def _():
                go(0, lat - 1, cot_bot, bot_recv)

        for step in range(1, n_lon):
            remote(cot_s.at[hop(step)], cot_r.at[lon], sent, near_recv, (lat, hop(step))).start()
        cot_r[lon] = cot_s[lon]
        send_edges(0)
        for step in range(n_lon // 2):
            other = 2 * wrap(lon // 2 + step, n_lon // 2)
            remote(
                cot_s.at[other], cot_r.at[n_lon + lon], sent, far_recv, (far_lat, other)
            ).start()

        loops(send_order[:ready], ship_step)
    with scope("prep2"):
        cut = 2 * (rounds // 4)
        loops(send_order[ready:cut], both_step)
        send_edges(1)
        loops(send_order[cut:], both_step)

    with scope("clear"):
        for s in range(2):
            for b in range(3):
                for i in (0, 1, tile_rows + 2, tile_rows + 3):
                    moved[s, b, i] = jnp.zeros((wide, channels), F32)
        dep[...] = jnp.zeros_like(dep)
        total[...] = jnp.zeros_like(total)
        bias[...] = jnp.zeros_like(bias)
        gka[...] = jnp.zeros_like(gka)

    def cot_wait(s):
        if s == 0:
            drain(cot_r.at[pl.ds(0, n_lon - 1)], near_recv)
        else:
            drain(cot_r.at[pl.ds(0, n_lon)], far_recv)

        @pl.when(tile_lat[s] > 0)
        def _():
            drain(cot_top.at[s], top_recv.at[s])

        @pl.when(tile_lat[s] < n_lat - 1)
        def _():
            drain(cot_bot.at[s], bot_recv.at[s])

    half = channels // 2
    for fetch in fetches[4:]:
        fetch.wait()
    tap = taps[...]

    def adjoint(h):
        c32[h, 0] = cot_top[h].astype(F32)
        c32[h, tile_rows + 1] = cot_bot[h].astype(F32)

        def widen(j, carry):
            at = h * n_lon + j
            ends = cot_r[at, own_rows * tile_cols:own_rows * tile_cols + EDGE, :].astype(F32)
            for r in range(own_rows):
                m = j * own_rows + r + 1
                c32[h, m, 0:tile_cols, :] = cot_r[at, r * tile_cols:(r + 1) * tile_cols, :].astype(F32)
                c32[h, m, tile_cols:wide, :] = pltpu.roll(ends, 2 * r, 0) if r else ends
            return carry

        lax.fori_loop(0, n_lon, widen, 0)

        def adjoin(m, carry):
            for c in range(0, channels, half):
                acc = jnp.zeros((tile_cols, half), F32)
                for a in (-1, 0, 1):
                    row = c32[h, m + 1 - a, :, c:c + half]
                    for b in (-1, 0, 1):
                        k = 3 * (a + 1) + b + 1
                        turned = pltpu.roll(row, b % wide, 0) if b else row
                        acc = acc + tap[k:k + 1, c:c + half] * turned[0:tile_cols]
                adj_f[pl.ds(pl.multiple_of(m * tile_cols, 8), tile_cols), c:c + half] = scale * acc
            return carry

        lax.fori_loop(0, tile_rows, adjoin, 0)
        adj_b[h] = adj_f[...].astype(BF16)

    def take(step, count):
        first, size = step * batch, count * batch
        s = first // peers
        with scope("rowwait"):
            drain(meta_r.at[pl.ds(first, size)], meta_recv.at[slot(step)])
            drain(rbuf.at[pl.ds(first, size)], row_recv.at[slot(step)])
        rows = jnp.concatenate([rbuf[first + q] for q in range(size)], axis=0)
        codes = jnp.concatenate([meta_r[first + q][:, 0:slots] for q in range(size)], axis=1)
        pick = (codes == iota((cells, size * slots), 0) + 1).astype(F32).astype(BF16)
        upstream = dot(pick, adj_b[s], ((0,), (0,))).astype(BF16)
        x = dot(rows, w_in[...]) + b_in[...]
        square = x * x
        t_val = jnp.tanh(x * (CURVE + (CURVE * BEND) * square))
        upper_half = 0.5 + 0.5 * t_val
        lower_half = 0.5 - 0.5 * t_val
        active = x * upper_half
        hidden = active.astype(BF16)
        slope = upper_half + (active * lower_half) * (2.0 * CURVE + (6.0 * CURVE * BEND) * square)
        encoded = dot(hidden, w_out[...]).astype(BF16)
        dep[s] += dot(pick, encoded)
        back = dot(upstream, w_out[...], ((1,), (1,)))
        pre = (back * slope).astype(BF16)
        total[0:hidden_size, :] += dot(hidden, upstream, ((0,), (0,)))
        total[hidden_size:hidden_size + feat, :] += dot(rows, pre, ((0,), (0,)))
        bias[...] += jnp.sum(pre.astype(F32), axis=0, keepdims=True)

    with scope("cotwaitA"):
        cot_wait(0)
    with scope("adjointA"):
        adjoint(0)

    part = rounds // 4

    def take_pair(g, carry):
        take(2 * part * g, 2 * part)
        return carry

    def take_one(g, carry):
        take(part * g, part)
        return carry

    with scope("take1"):
        lax.fori_loop(0, 1, take_pair, 0)
    with scope("adjointB"):
        @pl.when(dense)
        def _():
            with scope("cotwaitB"):
                cot_wait(1)
            adjoint(1)

        @pl.when(jnp.logical_not(dense))
        def _():
            adj_b[1] = adj_b[0]

    with scope("take2"):
        lax.fori_loop(1, 4 - LATE // 2, take_pair, 0)
    with scope("take3"):
        if LATE:
            lax.fori_loop(8 - LATE, 8, take_one, 0)

    with scope("rssend"):
        for p in range(n_lon):
            tot_b[p] = total[p * piece:(p + 1) * piece, :].astype(BF16)
        for step in range(1, n_lon):
            remote(tot_b.at[hop(step)], rs_r.at[lon], sent, rs_recv, (lat, hop(step))).start()

    def spread(h):
        def turn_row(m, carry):
            row = dep[h, pl.ds(pl.multiple_of(m * tile_cols, 8), tile_cols), :]
            row = jnp.concatenate([row, jnp.zeros((EDGE, channels), F32)], axis=0)
            moved[h, 0, m + 2] = pltpu.roll(row, 1, 0)
            moved[h, 1, m + 2] = row
            moved[h, 2, m + 2] = pltpu.roll(row, wide - 1, 0)
            return carry

        lax.fori_loop(0, tile_rows, turn_row, 0)

        def out_row(i, c):
            acc = jnp.zeros((wide, half), F32)
            seen = c32[h, i, :, c:c + half]
            for a in (-1, 0, 1):
                for b in (-1, 0, 1):
                    k = 3 * (a + 1) + b + 1
                    value = moved[h, b + 1, i + 1 + a, :, c:c + half]
                    acc = acc + tap[k:k + 1, c:c + half] * value
                    prod = seen * value
                    folded = prod[0:8]
                    for at in range(8, wide, 8):
                        folded = folded + prod[at:at + 8]
                    gka[k, :, c:c + half] += folded
            return acc

        def strip(j, carry):
            for c in range(0, channels, half):
                mixed = jnp.zeros((EDGE, half), F32)
                for r in range(own_rows):
                    acc = out_row(j * own_rows + r + 1, c)
                    con_s[h, j, r * tile_cols:(r + 1) * tile_cols, c:c + half] = acc[0:tile_cols].astype(BF16)
                    ends = acc[tile_cols:wide]
                    mixed = mixed + (pltpu.roll(ends, EDGE - 2 * r, 0) if r else ends)
                con_s[h, j, own_rows * tile_cols:own_rows * tile_cols + EDGE, c:c + half] = mixed.astype(BF16)
            return carry

        for e, i in ((0, 0), (1, tile_rows + 1)):
            for c in range(0, channels, half):
                con_e[h, e, :, c:c + half] = out_row(i, c).astype(BF16)
        lax.fori_loop(0, n_lon, strip, 0)

    def send_strip(h, step):
        where = lon if h == 0 else n_lon + lon // 2
        remote(
            con_s.at[h, hop(step)], main_o.at[where], sent, con_recv, (tile_lat[h], hop(step))
        ).start()

    def rim_copy(h, e):
        where = lon if h == 0 else n_lon + lon // 2
        if e == 0:
            return remote(con_e.at[h, 0], bot_o.at[where], sent, rim_recv, (tile_lat[h] - 1, n_lon - 1))
        return remote(con_e.at[h, 1], top_o.at[where], sent, rim_recv, (tile_lat[h] + 1, 0))

    def rims(h, act):
        @pl.when(tile_lat[h] > 0)
        def _():
            act(rim_copy(h, 0))

        @pl.when(tile_lat[h] < n_lat - 1)
        def _():
            act(rim_copy(h, 1))

    first_part = n_lon // 2
    with scope("spread"):
        @pl.when(dense)
        def _():
            spread(1)
            rims(1, lambda copy: copy.start())
            for step in range(first_part):
                send_strip(1, step)

        @pl.when(jnp.logical_not(dense))
        def _():
            dep[0] += dep[1]

        spread(0)
        rims(0, lambda copy: copy.start())

    with scope("misc"):
        grads = [jnp.sum(gka[k], axis=0, keepdims=True) * scale for k in range(len(OFFSETS))]
        spare = misc_s.shape[0] - len(OFFSETS) - 1
        misc_s[...] = jnp.concatenate(
            [bias[...]] + grads + [jnp.zeros((spare, channels), F32)], axis=0
        ).astype(BF16)
        for step in range(1, n_lon):
            remote(misc_s, misc_r.at[lon], sent, mp_recv, (lat, hop(step))).start()
        misc_r[lon] = misc_s[...]

    with scope("rswait"):
        drain(rs_r.at[pl.ds(0, n_lon - 1)], rs_recv)
    with scope("zsend"):
        rs_r[lon] = tot_b[lon]
        part = rs_r[0].astype(F32)
        for p in range(1, n_lon):
            part = part + rs_r[p].astype(F32)
        z_s[...] = part.astype(BF16)
        for step in range(1, n_lat):
            remote(z_s, z_r.at[lat], sent, z_recv, (wrap(lat + step, n_lat), lon)).start()
        z_r[lat] = z_s[...]

        @pl.when(dense)
        def _():
            for step in range(first_part, n_lon):
                send_strip(1, step)

        for step in range(1, n_lon):
            send_strip(0, step)
        main_o[lon] = con_s[0, lon]

    with scope("miscz"):
        drain(misc_r.at[pl.ds(0, n_lon - 1)], mp_recv)
        part = misc_r[0].astype(F32)
        for p in range(1, n_lon):
            part = part + misc_r[p].astype(F32)
        misc_z[...] = part.astype(BF16)
        for step in range(1, n_lat):
            remote(misc_z, misc_o.at[lat], sent, mz_recv, (wrap(lat + step, n_lat), lon)).start()
        misc_o[lat] = misc_z[...]

    with scope("zwait"):
        drain(z_r.at[pl.ds(0, n_lat - 1)], z_recv)
    with scope("agsend"):
        part = z_r[0].astype(F32)
        for p in range(1, n_lat):
            part = part + z_r[p].astype(F32)
        fin_s[...] = part.astype(BF16)
        for step in range(1, n_lon):
            remote(fin_s, sums_o.at[lon], sent, ag_recv, (lat, hop(step))).start()
        sums_o[lon] = fin_s[...]

    with scope("mzwait"):
        drain(misc_o.at[pl.ds(0, n_lat - 1)], mz_recv)
    with scope("conwait"):
        drain(main_o.at[pl.ds(0, holders - 1)], con_recv)

        @pl.when(has_top)
        def _():
            drain(top_o, rim_recv)

        @pl.when(has_bot)
        def _():
            drain(bot_o, rim_recv)
    with scope("grid"):
        value = misc_o[0].astype(F32)
        for z in range(1, n_lat):
            value = value + misc_o[z].astype(F32)
        gb_o[...] = value[0:1]
        gk_o[...] = value[1:1 + len(OFFSETS)]
        here = iota((tile_cols, channels), 0)

        def both(ref, j):
            value = ref[j].astype(F32)
            return value if j % 2 else value + ref[n_lon + j // 2].astype(F32)

        bodies = []
        for j in range(n_lon):
            value = both(main_o, j)
            ends = value[own_rows * tile_cols:own_rows * tile_cols + EDGE]
            rows = []
            for y in range(own_rows):
                body = value[y * tile_cols:(y + 1) * tile_cols]
                right = ends[(EDGE - 2 * y) % EDGE:(EDGE - 2 * y) % EDGE + 1]
                left = ends[EDGE - 1 - 2 * y:EDGE - 2 * y]
                for y_at, source in ((0, top_o), (own_rows - 1, bot_o)):
                    if y == y_at:
                        extra = both(source, j)
                        body = body + extra[0:tile_cols]
                        right = right + extra[tile_cols:tile_cols + 1]
                        left = left + extra[tile_cols + EDGE - 1:tile_cols + EDGE]
                rows.append((body, right, left))
            bodies.append(rows)
        for j in range(n_lon):
            for y in range(own_rows):
                value = bodies[j][y][0]
                value = value + jnp.where(here == 0, bodies[(j - 1) % n_lon][y][1], 0.0)
                value = value + jnp.where(here == tile_cols - 1, bodies[(j + 1) % n_lon][y][2], 0.0)
                grid_o[y, j * tile_cols:(j + 1) * tile_cols, :] = value.astype(BF16)
    with scope("agwait"):
        drain(sums_o.at[pl.ds(0, n_lon - 1)], ag_recv)
    with scope("sums"):
        for p in range(n_lon):
            value = sums_o[p].astype(F32)
            start = p * piece
            for ref, low, high in ((gout_o, 0, hidden_size), (gin_o, hidden_size, n_lon * piece)):
                begin, end = max(start, low), min(start + piece, high)
                if begin < end:
                    ref[begin - low:end - low, :] = value[begin - start:end - start]

    with scope("final"):
        drain(sbuf.at[pl.ds(0, 2 * peers - 2)], sent)
        drain(meta_r.at[pl.ds(0, 2 * peers - 2)], sent)

        @pl.when(jnp.logical_not(dense))
        def _():
            drain(sbuf.at[0], sent)
            drain(meta_r.at[0], sent)

        drain(cot_r.at[pl.ds(0, holders - 1)], sent)

        @pl.when(jnp.logical_and(lon == n_lon - 1, lat < n_lat - 1))
        def _():
            drain(top_o, sent)

        @pl.when(jnp.logical_and(lon == 0, lat > 0))
        def _():
            drain(top_o, sent)

        drain(main_o.at[pl.ds(0, n_lon - 1)], sent)
        rims(0, lambda copy: copy.wait_send())

        @pl.when(dense)
        def _():
            drain(main_o.at[pl.ds(0, n_lon)], sent)
            rims(1, lambda copy: copy.wait_send())

        drain(rs_r.at[pl.ds(0, n_lon - 1)], sent)
        drain(misc_r.at[pl.ds(0, n_lon - 1)], sent)
        drain(z_r.at[pl.ds(0, n_lat - 1)], sent)
        drain(misc_o.at[pl.ds(0, n_lat - 1)], sent)
        drain(sums_o.at[pl.ds(0, n_lon - 1)], sent)


def finish(*refs):
    sem, half = refs[-1], (len(refs) - 1) // 2
    copies = [pltpu.make_async_copy(refs[i], refs[half + i], sem) for i in range(half)]
    for copy in copies:
        copy.start()
    for copy in copies:
        copy.wait()


def local(
    observations, owner_device, local_cell, valid_counts,
    weight_in, bias_in, weight_out, kernel_taps, cotangent,
):
    n_lat, n_lon = lax.axis_size("lat"), lax.axis_size("lon")
    n = n_lat * n_lon
    obs_rows, feat = observations.shape
    hidden_size, channels = weight_out.shape
    own_rows, cols, _ = cotangent.shape
    tile_rows, tile_cols = own_rows * n_lon, cols // n_lon
    cells = tile_rows * tile_cols
    slots = round_up(2 * obs_rows // n, 16)
    batch = 4 if slots > 48 else 8
    piece = (hidden_size + feat) // n_lon
    taps = kernel_taps.shape[0]
    misc_rows = round_up(taps + 1, 16)
    peers = n // 2
    holders = n_lon + n_lon // 2
    strip_rows = own_rows * tile_cols + EDGE
    wide = tile_cols + EDGE
    scale = 1.0 / math.sqrt(obs_rows * n)
    results = (
        (cotangent.shape, BF16), ((feat, hidden_size), F32), ((1, hidden_size), F32),
        ((hidden_size, channels), F32), ((taps, channels), F32),
    )
    far = functools.partial(pltpu.with_memory_space_constraint, memory_space=pltpu.HBM)
    hbm = pl.BlockSpec(memory_space=pltpu.HBM)
    vmem = pl.BlockSpec(memory_space=pltpu.VMEM)
    dma = pltpu.SemaphoreType.DMA
    V = pltpu.VMEM
    found = pl.pallas_call(
        functools.partial(kernel, n_lat, n_lon, slots, batch, scale),
        out_shape=tuple(V(shape, kind) for shape, kind in results),
        in_specs=[hbm, hbm, hbm, pl.BlockSpec(memory_space=pltpu.SMEM)] + [hbm] * 5,
        out_specs=(vmem,) * 5,
        scratch_shapes=[
            V((obs_rows, feat), BF16), V((1, obs_rows), jnp.int32), V((obs_rows // 128, 128), jnp.int32),
            V((feat, hidden_size), BF16), V((1, hidden_size), F32), V((hidden_size, channels), BF16),
            V((taps, channels), F32), V((own_rows, cols, channels), BF16),
            V((holders, strip_rows, channels), BF16), V((holders, wide, channels), BF16),
            V((holders, wide, channels), BF16), V((n_lon, piece, channels), BF16),
            V((n_lat, misc_rows, channels), BF16),
            V((n, 1, 128), jnp.int32), V((n, 1, 128), jnp.int32), V((1, obs_rows), jnp.int32),
            V((n, slots, feat), BF16), V((n, slots, feat), BF16),
            V((n_lon, strip_rows, channels), BF16), V((2, n_lon, wide, channels), BF16),
            V((2 * n_lon, strip_rows, channels), BF16), V((2, wide, channels), BF16), V((2, wide, channels), BF16),
            V((2, tile_rows + 2, wide, channels), F32), V((cells, channels), F32), V((2, cells, channels), BF16),
            V((2, cells, channels), F32), V((2, 3, tile_rows + 4, wide, channels), F32),
            V((2, n_lon, strip_rows, channels), BF16), V((2, 2, wide, channels), BF16),
            V((taps, 8, channels), F32), V((hidden_size + feat, channels), F32), V((1, hidden_size), F32),
            V((n_lon, piece, channels), BF16), V((n_lon, piece, channels), BF16),
            V((piece, channels), BF16), V((n_lat, piece, channels), BF16), V((piece, channels), BF16),
            V((misc_rows, channels), BF16), V((n_lon, misc_rows, channels), BF16), V((misc_rows, channels), BF16),
            dma((5,)), dma, dma((4 + LATE // 2,)), dma((4 + LATE // 2,)), dma, dma, dma((2,)), dma((2,)),
            dma, dma, dma, dma, dma, dma, dma,
        ],
        compiler_params=pltpu.CompilerParams(
            collective_id=0, has_side_effects=True, vmem_limit_bytes=48 * 1024 * 1024
        ),
    )(
        far(observations), far(owner_device.reshape(1, obs_rows)), far(local_cell.reshape(obs_rows // 128, 128)),
        valid_counts, far(weight_in), far(bias_in.reshape(1, hidden_size)), far(weight_out), far(kernel_taps),
        far(cotangent),
    )
    grid_out, grad_in, grad_bias, grad_out, grad_kernel = pl.pallas_call(
        finish,
        out_shape=tuple(jax.ShapeDtypeStruct(shape, kind) for shape, kind in results),
        in_specs=[vmem] * 5,
        out_specs=(hbm,) * 5,
        scratch_shapes=[dma],
    )(*[pltpu.with_memory_space_constraint(value, pltpu.VMEM) for value in found])
    return (grid_out, grad_in, grad_bias.reshape(hidden_size), grad_out, grad_kernel)


def solution(mesh):
    return jax.shard_map(
        local,
        mesh=mesh,
        in_specs=(
            P(("lat", "lon"), None),
            P(("lat", "lon"), None),
            P(("lat", "lon")),
            P(("lat", "lon")),
            P(),
            P(),
            P(),
            P(),
            P(("lat", "lon"), None, None),
        ),
        out_specs=(P(("lat", "lon"), None, None), P(), P(), P(), P()),
        check_vma=False,
    )
```
